128 devices in a mesh: emb: 32 (over z, x, core), seq: 4 (over y).
Axes of the slice: x: 4, y: 4, z: 4, core: 2. Of those that a mesh axis runs over, the one named last changes fastest.
Arguments:
- item_table: bfloat16 [131072, 512], P('emb'), may hold values from -6 to 6
- fetch_rows: int32 [32, 4, 32, 16], P('emb', 'seq'), may hold values from 0 to 4095
- event_slot: int32 [131072], P(('emb', 'seq')), may hold values from 0 to 511, as said below
- lengths: int32 [128, 8], P(('emb', 'seq')), may hold values from 1 to 512, 1024 in all within a row
- in_weight: bfloat16 [512, 2048], replicated, may hold values from -0.25 to 0.25
- out_weight: bfloat16 [512, 512], replicated, may hold values from -0.25 to 0.25
- out_grad: bfloat16 [131072, 512], P(('emb', 'seq')), may hold values from -6 to 6
Outputs:
- layer_out: bfloat16 [131072, 512], P(('emb', 'seq'))
- table_grad: float32 [131072, 512], P(('emb', 'seq'))
- in_weight_grad: float32 [512, 2048], replicated
- out_weight_grad: float32 [512, 512], replicated
The draws below stay inside these ranges and needn't reach their ends.
Inputs may be any that keep to these rules, and one draw needn't show every extreme that they name: `event_slot`: within each buffer of 1024 events every slot 0 to 511 is named by at least one event.
All inputs are finite; a program needn't handle non-finite values.
Results may differ from the reference program's by a relative error of at most 0.02.
Values may be sent and summed in bfloat16 or wider, within the bound.
A program may use at most 192 MiB of HBM per device.

```python
import math
import jax
import jax.numpy as jnp
import numpy as np
from jax import lax

D = 512
HEADS = 4
TOK_DEV = 1024
SEQ_DEV = 8
MOST = 512
SLOTS = 512
CAP = 16
R_SHARD = 4096
ROWS = 131072
BUFFERS = 128
TOKENS = 131072
N_EMB = 32
N_SEQ = 4


def draw_event_slot(key, part):
    buffer_keys = jax.random.split(jax.random.fold_in(key, 17), BUFFERS)

    def one_buffer(buffer_key):
        first_key, second_key, third_key = jax.random.split(buffer_key, 3)
        covered = jax.random.permutation(first_key, SLOTS).astype(jnp.int32)
        repeats = jax.random.randint(second_key, (TOK_DEV - SLOTS,), 0, SLOTS).astype(jnp.int32)
        joined = jnp.concatenate([covered, repeats])
        return jax.random.permutation(third_key, joined).astype(jnp.int32)
    return jax.vmap(one_buffer)(buffer_keys).reshape(TOKENS).astype(jnp.int32)


def with_ends(array, rng, least, largest):
    extent = array.shape
    place = [jax.random.randint(jax.random.fold_in(rng, axis), (), 0, extent[axis]) for axis in range(len(extent))]
    array = array.at[tuple(place)].set(least)
    longest = extent.index(max(extent))
    place[longest] = (place[longest] + 1) % extent[longest]
    return array.at[tuple(place)].set(largest)


def levels(own_key, dims, cuts, low, high):
    def one(position, shards_of):
        draws = jax.random.uniform(jax.random.fold_in(jax.random.fold_in(own_key, 6), position), (shards_of,), jnp.float32, low / len(cuts), high / len(cuts))
        return jnp.repeat(jnp.exp(draws), dims[position] // shards_of).reshape((-1,) + (1,) * (len(dims) - position - 1))

    level = one(*cuts[0])
    for cut in cuts[1:]:
        level = level * one(*cut)
    return level


def length_profile(amount, total, limit, lean):
    weights = [(1 << 20) // math.isqrt(grade ** lean) + 1 for grade in range(2, amount + 1)]
    rest, given = total - limit - (amount - 1), [1] * (amount - 1)
    while rest > 0:
        free = [i for i in range(amount - 1) if given[i] < limit]
        pool, left = sum([weights[i] for i in free]), rest
        for i in free:
            addition = min(limit - given[i], max(1, left * weights[i] // pool), rest)
            given[i] = given[i] + addition
            rest = rest - addition
    return np.array([limit] + given)


def ragged_sizes(own_key, number_of, total, most, slope):
    if number_of == 2:
        one = jax.random.randint(own_key, (), max(1, total - most), min(most, total - 1) + 1)
        return jnp.stack([one, total - one])
    sizes = jnp.asarray(length_profile(number_of, total, most, slope), jnp.int32)
    couples = (number_of - 1) // 2
    source_of, taker = sizes[1:1 + 2 * couples:2], sizes[2:2 + 2 * couples:2]
    margin = jnp.minimum(source_of - 1, most - taker)
    moved = jax.random.randint(jax.random.fold_in(own_key, 1), (couples,), 0, 1 << 20) % (margin + 1)
    sizes = sizes.at[1:1 + 2 * couples:2].set(source_of - moved).at[2:2 + 2 * couples:2].set(taker + moved)
    return sizes[jax.random.permutation(jax.random.fold_in(own_key, 2), number_of)]


def bell_draw(key, shape, scale, bound, cuts=(), kind=jnp.bfloat16):
    drawn = jax.random.normal(key, shape, jnp.float32) * scale
    if len(cuts) > 0:
        drawn = levels(key, shape, cuts, -0.22, 0.18) * drawn
    return jnp.clip(drawn, min=-bound, max=bound).astype(kind)


def setup_inputs(seed: int = 0) -> dict:
    splits = jax.random.split(jax.random.key(seed), 8)
    item_table = bell_draw(splits[0], (ROWS, D), 1.0, 6.0, ((0, 32),))
    fetch_rows = with_ends(jax.random.randint(splits[1], (N_EMB, N_SEQ, N_EMB, CAP), 0, R_SHARD), jax.random.fold_in(splits[1], 1), 0, R_SHARD - 1).astype(jnp.int32)
    event_slot = draw_event_slot(jax.random.fold_in(splits[7], 71), 0)
    lengths = jax.vmap(lambda own: ragged_sizes(own, SEQ_DEV, TOK_DEV, MOST, 2))(jax.random.split(splits[3], BUFFERS)).reshape((BUFFERS, SEQ_DEV)).astype(jnp.int32)
    in_weight = bell_draw(splits[4], (D, 4 * D), D ** -0.5, 0.25)
    out_weight = bell_draw(splits[5], (D, D), D ** -0.5, 0.25)
    out_grad = bell_draw(splits[6], (TOKENS, D), 1.0, 6.0, ((0, 128),))
    return dict(item_table=item_table, fetch_rows=fetch_rows, event_slot=event_slot, lengths=lengths, in_weight=in_weight, out_weight=out_weight, out_grad=out_grad)


EPS = 1e-05

def normalize(rows_in):
    center = rows_in - lax.optimization_barrier(jnp.mean(rows_in, axis=-1, keepdims=True))
    spread = lax.optimization_barrier(jnp.mean(center * center, axis=-1, keepdims=True))
    return center * lax.rsqrt(spread + EPS)

def hstu_layer(events, in_weight, out_weight, lengths_row):
    rows_count, model_width = events.shape
    head_size = model_width // HEADS
    normed = normalize(events.astype(jnp.float32)).astype(jnp.bfloat16)
    hidden = jax.nn.silu(jnp.dot(normed, in_weight, preferred_element_type=jnp.float32))
    update_gate = hidden[:, :model_width]
    values = hidden[:, model_width:2 * model_width].astype(jnp.bfloat16).reshape(rows_count, HEADS, head_size)
    queries = hidden[:, 2 * model_width:3 * model_width].astype(jnp.bfloat16).reshape(rows_count, HEADS, head_size)
    key_rows = hidden[:, 3 * model_width:].astype(jnp.bfloat16).reshape(rows_count, HEADS, head_size)
    scores = jnp.einsum('ihd,jhd->hij', queries, key_rows, preferred_element_type=jnp.float32) * head_size ** (-0.5)
    places = jnp.arange(rows_count, dtype=jnp.int32)
    seq_ends = jnp.cumsum(lengths_row).astype(jnp.int32)
    segment = lax.optimization_barrier(jnp.sum((places[:, None] >= seq_ends[None, :]).astype(jnp.int32), axis=1))
    allowed = (segment[:, None] == segment[None, :]) & (places[None, :] <= places[:, None])
    weights = jnp.where(allowed[None], jax.nn.silu(scores) / MOST, 0.0).astype(jnp.bfloat16)
    attended = jnp.einsum('hij,jhd->ihd', weights, values, preferred_element_type=jnp.float32).reshape(rows_count, model_width)
    gated_rows = (normalize(attended) * update_gate).astype(jnp.bfloat16)
    return (jnp.dot(gated_rows, out_weight, preferred_element_type=jnp.float32) + events.astype(jnp.float32)).astype(jnp.bfloat16)

def reference(item_table, fetch_rows, event_slot, lengths, in_weight, out_weight, out_grad):
    owners = (jnp.arange(SLOTS, dtype=jnp.int32) // CAP * R_SHARD).astype(jnp.int32)
    slot_rows = (fetch_rows.reshape(BUFFERS, SLOTS) + owners[None, :]).astype(jnp.int32)
    event_rows = jnp.take_along_axis(slot_rows, event_slot.reshape(BUFFERS, TOK_DEV).astype(jnp.int32), axis=1).astype(jnp.int32)
    events = item_table[event_rows]

    def one_buffer(totals, pieces):
        rows_in, lengths_row, grad_row = pieces

        def forward(rows_x, first, second):
            return hstu_layer(rows_x, first, second, lengths_row)
        result, pullback = jax.vjp(forward, rows_in, in_weight, out_weight)
        row_grad, first_grad, second_grad = pullback(grad_row)
        totals = (totals[0] + first_grad.astype(jnp.float32), totals[1] + second_grad.astype(jnp.float32))
        return (totals, (result, row_grad))
    start = (jnp.zeros((D, 4 * D), jnp.float32), jnp.zeros((D, D), jnp.float32))
    totals, outputs = lax.scan(one_buffer, start, (events, lengths, out_grad.reshape(BUFFERS, TOK_DEV, D)))
    results, row_grads = outputs
    table_grad = jax.ops.segment_sum(row_grads.reshape(TOKENS, D).astype(jnp.float32), event_rows.reshape(TOKENS), num_segments=ROWS)
    return (results.reshape(TOKENS, D), table_grad, totals[0], totals[1])
```

```python
import functools, math
import jax, jax.numpy as jnp
from jax import lax
from jax.experimental import pallas as pl
from jax.experimental.pallas import tpu as pltpu
from jax.sharding import PartitionSpec as P

F32, BF16 = jnp.float32, jnp.bfloat16
EPS = 1e-05
MOST = 512
B = 256
LAST = (((1,), (1,)), ((), ()))


def rows_at(i):
    return pl.ds(pl.multiple_of(i * B, B), B)


def expand(ev_ref, tab_ref, events_s, pick_s):
    slots = tab_ref.shape[0]
    ev = ev_ref[...]
    ev_t = jnp.transpose(ev)
    lane = lax.broadcasted_iota(jnp.int32, (128, slots), 1)
    sub = lax.broadcasted_iota(jnp.int32, (slots, 128), 0)
    for a in range(ev.shape[0]):
        hot = jnp.where(ev_t[:, a : a + 1] == lane, 1.0, 0.0).astype(BF16)
        events_s[128 * a : 128 * a + 128, :] = jnp.dot(
            hot, tab_ref[...], preferred_element_type=F32
        ).astype(BF16)
        pick_s[:, 128 * a : 128 * a + 128] = jnp.where(sub == ev[a : a + 1, :], 1.0, 0.0).astype(
            BF16
        )


def project(r, events_s, win_ref, normed_s, normed_t, rstd_s, gate_s, dsil_s, qkv_s, kv_t):
    rows = rows_at(r)
    width = events_s.shape[1]
    e = events_s[rows, :].astype(F32)
    c = e - jnp.mean(e, axis=-1, keepdims=True)
    rs = lax.rsqrt(jnp.mean(c * c, axis=-1, keepdims=True) + EPS)
    n = (c * rs).astype(BF16)
    normed_s[rows, :] = n
    rstd_s[rows, :] = rs
    normed_t[:, rows] = jnp.transpose(n)
    for b in range(4):
        cols = slice(b * width, (b + 1) * width)
        x = jnp.dot(n, win_ref[:, cols], preferred_element_type=F32)
        hx = 0.5 * x
        t = jnp.tanh(hx)
        u = 1.0 + t
        y = hx * u
        dsil_s[rows, cols] = (0.5 * (u + hx * (1.0 - t * t))).astype(BF16)
        if b == 0:
            gate_s[rows, :] = y
        else:
            yb = y.astype(BF16)
            qkv_s[b - 1, rows, :] = yb
            if b == 1:
                kv_t[1, :, rows] = jnp.transpose(yb)
            elif b == 3:
                kv_t[0, :, rows] = jnp.transpose(yb)


def pairs(blocks):
    back = MOST // B
    return [(q, k) for q in range(blocks) for k in range(max(0, q - back), q + 1)]


def attend(h, starts, qkv_s, kv_t, att_t, p_s, d_s, blocks):
    hc = pl.ds(pl.multiple_of(h * 128, 128), 128)
    lane = lax.broadcasted_iota(jnp.int32, (B, B), 1)
    sub = lax.broadcasted_iota(jnp.int32, (B, B), 0)
    head = 128
    c1 = 0.5 / math.sqrt(head)
    total = None
    for i, (q, k) in enumerate(pairs(blocks)):
        kk = qkv_s[2, k * B : (k + 1) * B, hc]
        qq = qkv_s[1, q * B : (q + 1) * B, hc]
        x = lax.dot_general(kk, qq, LAST, preferred_element_type=F32)
        hh = x * c1
        t = jnp.tanh(hh)
        u = 1.0 + t
        mask = (sub + k * B) >= starts[q]
        if q == k:
            mask = mask & (sub <= lane)
        w = jnp.where(mask, (hh * u) * (1.0 / MOST), 0.0).astype(BF16)
        d = jnp.where(mask, (u + hh * (1.0 - t * t)) * (c1 / MOST), 0.0).astype(BF16)
        p_s[h, i] = w
        d_s[h, i] = d
        o = jnp.dot(kv_t[1, hc, k * B : (k + 1) * B], w, preferred_element_type=F32)
        total = o if k == max(0, q - MOST // B) else total + o
        if q == k:
            att_t[hc, q * B : (q + 1) * B] = total


def middle(r, att_t, gate_s, dsil_s, events_s, wout_ref, og_ref, lo_ref, gated_t, dx_s, do_s):
    rows = rows_at(r)
    width = events_s.shape[1]
    a = jnp.transpose(att_t[:, rows])
    c = a - jnp.mean(a, axis=-1, keepdims=True)
    rs = lax.rsqrt(jnp.mean(c * c, axis=-1, keepdims=True) + EPS)
    xh = c * rs
    gate = gate_s[rows, :]
    gated = (xh * gate).astype(BF16)
    out = jnp.dot(gated, wout_ref[...], preferred_element_type=F32)
    lo_ref[rows, :] = (out + events_s[rows, :].astype(F32)).astype(BF16)
    gated_t[:, rows] = jnp.transpose(gated)
    og = og_ref[rows, :]
    dg = lax.dot_general(og, wout_ref[...], LAST, preferred_element_type=F32)
    dg = dg.astype(BF16).astype(F32)
    dx_s[rows, :width] = (dg * xh * dsil_s[rows, :width].astype(F32)).astype(BF16)
    dxh = dg * gate
    m1 = jnp.mean(dxh, axis=-1, keepdims=True)
    m2 = jnp.mean(dxh * xh, axis=-1, keepdims=True)
    do_s[rows, :] = (rs * (dxh - m1 - xh * m2)).astype(BF16)


def attend_back(h, qkv_s, kv_t, p_s, d_s, do_s, dsil_s, dx_s, dq_t, blocks, width):
    hc = pl.ds(pl.multiple_of(h * 128, 128), 128)

    def put(block, part, grad):
        cols = pl.ds(pl.multiple_of(part * width + h * 128, 128), 128)
        rows = slice(block * B, (block + 1) * B)
        dx_s[rows, cols] = (
            grad.astype(BF16).astype(F32) * dsil_s[rows, cols].astype(F32)
        ).astype(BF16)

    order = pairs(blocks)
    for k in range(blocks):
        dv = dk = None
        vv = qkv_s[0, k * B : (k + 1) * B, hc]
        for q in range(k, min(k + MOST // B, blocks - 1) + 1):
            i = order.index((q, k))
            do = do_s[q * B : (q + 1) * B, hc]
            dp = lax.dot_general(vv, do, LAST, preferred_element_type=F32).astype(BF16)
            ds = dp * d_s[h, i]
            dv1 = jnp.dot(p_s[h, i], do, preferred_element_type=F32)
            dk1 = jnp.dot(ds, qkv_s[1, q * B : (q + 1) * B, hc], preferred_element_type=F32)
            dv = dv1 if dv is None else dv + dv1
            dk = dk1 if dk is None else dk + dk1
            dq1 = jnp.dot(kv_t[0, hc, k * B : (k + 1) * B], ds, preferred_element_type=F32)
            at = slice(q * B, (q + 1) * B)
            if k == max(0, q - MOST // B):
                dq_t[:, at] = dq1
            else:
                dq_t[:, at] += dq1
        put(k, 1, dv)
        put(k, 3, dk)
    for q in range(blocks):
        put(q, 2, jnp.transpose(dq_t[:, q * B : (q + 1) * B]))


def event_back(r, dx_s, win_ref, normed_s, rstd_s, og_ref, eg_s):
    rows = rows_at(r)
    g = lax.dot_general(dx_s[rows, :], win_ref[...], LAST, preferred_element_type=F32)
    g = g.astype(BF16).astype(F32)
    xh = normed_s[rows, :].astype(F32)
    m1 = jnp.mean(g, axis=-1, keepdims=True)
    m2 = jnp.mean(g * xh, axis=-1, keepdims=True)
    de = (rstd_s[rows, :] * (g - m1 - xh * m2)).astype(BF16)
    eg_s[rows, :] = (de.astype(F32) + og_ref[rows, :].astype(F32)).astype(BF16)


def row_starts(len_ref, blocks):
    ends, at = [], jnp.int32(0)
    for s in range(len_ref.shape[1]):
        at = at + len_ref[0, s]
        ends.append(at)
    starts = []
    for q in range(blocks):
        place = lax.broadcasted_iota(jnp.int32, (1, B), 1) + q * B
        start = jnp.zeros((1, B), jnp.int32)
        for e in ends:
            start = jnp.where(place >= e, e, start)
        starts.append(start)
    return starts


def compute(len_ref, ev_ref, tab_ref, win_ref, wout_ref, og_ref, lo_ref, sg_ref, g_ref,
            events_s, pick_s, normed_s, normed_t, rstd_s, gate_s, dsil_s, qkv_s, kv_t,
            att_t, p_s, d_s, gated_t, dx_s, do_s, dq_t, eg_s):
    tokens, width = og_ref.shape
    blocks = tokens // B
    heads = width // 128
    expand(ev_ref, tab_ref, events_s, pick_s)
    pl.loop(0, blocks)(lambda r: project(
        r, events_s, win_ref, normed_s, normed_t, rstd_s, gate_s, dsil_s, qkv_s, kv_t))
    starts = row_starts(len_ref, blocks)
    pl.loop(0, heads)(lambda h: attend(h, starts, qkv_s, kv_t, att_t, p_s, d_s, blocks))
    pl.loop(0, blocks)(lambda r: middle(
        r, att_t, gate_s, dsil_s, events_s, wout_ref, og_ref, lo_ref, gated_t, dx_s, do_s))

    def put_grad(c, val):
        g_ref[pl.ds(c * 64, 32)] = val[:, :128].astype(BF16).reshape(32, 16, 128)
        g_ref[pl.ds(c * 64 + 32, 32)] = val[:, 128:].astype(BF16).reshape(32, 16, 128)

    for c in range(2):
        put_grad(8 + c, jnp.dot(gated_t[...], og_ref[:, c * B : (c + 1) * B],
                                preferred_element_type=F32))
    pl.loop(0, heads)(lambda h: attend_back(
        h, qkv_s, kv_t, p_s, d_s, do_s, dsil_s, dx_s, dq_t, blocks, width))
    pl.loop(0, blocks)(lambda r: event_back(r, dx_s, win_ref, normed_s, rstd_s, og_ref, eg_s))
    sg_ref[...] = jnp.dot(pick_s[...], eg_s[...], preferred_element_type=F32).astype(BF16)

    @pl.loop(0, 8)
    def _(c):
        cols = pl.ds(pl.multiple_of(c * B, B), B)
        put_grad(c, jnp.dot(normed_t[...], dx_s[:, cols], preferred_element_type=F32))


def compute_scratch(tokens, width, slots):
    n = len(pairs(tokens // B))
    heads = width // 128
    return [
        pltpu.VMEM((tokens, width), BF16),
        pltpu.VMEM((slots, tokens), BF16),
        pltpu.VMEM((tokens, width), BF16),
        pltpu.VMEM((width, tokens), BF16),
        pltpu.VMEM((tokens, 1), F32),
        pltpu.VMEM((tokens, width), F32),
        pltpu.VMEM((tokens, 4 * width), BF16),
        pltpu.VMEM((3, tokens, width), BF16),
        pltpu.VMEM((2, width, tokens), BF16),
        pltpu.VMEM((width, tokens), F32),
        pltpu.VMEM((heads, n, B, B), BF16),
        pltpu.VMEM((heads, n, B, B), BF16),
        pltpu.VMEM((width, tokens), BF16),
        pltpu.VMEM((tokens, 4 * width), BF16),
        pltpu.VMEM((tokens, width), BF16),
        pltpu.VMEM((128, tokens), F32),
        pltpu.VMEM((tokens, width), BF16),
    ]


def local_layer(lengths, ev, tab, win, wout, og):
    tokens, width = og.shape
    slots = tab.shape[0]
    vm = pl.BlockSpec(memory_space=pltpu.VMEM)
    return pl.pallas_call(
        compute,
        name="layer",
        out_shape=(
            jax.ShapeDtypeStruct((tokens, width), BF16),
            jax.ShapeDtypeStruct((slots, width), BF16),
            jax.ShapeDtypeStruct((640, 16, 128), BF16),
        ),
        in_specs=[pl.BlockSpec(memory_space=pltpu.SMEM)] + [vm] * 5,
        out_specs=(vm, vm, vm),
        scratch_shapes=compute_scratch(tokens, width, slots),
        compiler_params=pltpu.CompilerParams(vmem_limit_bytes=64000000),
        cost_estimate=pl.CostEstimate(flops=14 * 10**9, bytes_accessed=8 * 10**6, transcendentals=6 * 10**6),
    )(lengths, ev, tab, win, wout, og)


MESH = pl.DeviceIdType.MESH


def remote(src, dst, send_sem, recv_sem, emb, seq):
    return pltpu.make_async_remote_copy(
        src_ref=src, dst_ref=dst, send_sem=send_sem, recv_sem=recv_sem,
        device_id=(emb, seq), device_id_type=MESH,
    )


def greet(peers):
    barrier = pltpu.get_barrier_semaphore()
    for emb, seq in peers:
        pl.semaphore_signal(barrier, inc=1, device_id=(emb, seq), device_id_type=MESH)
    pl.semaphore_wait(barrier, len(peers))


def fetch(n_emb, n_seq, req_ref, table_ref, tab_ref, idx_ref, table_v, rows_v, load_sem,
          i_send, i_recv, y_send, y_recv, r_send, r_recv):
    e, s = lax.axis_index("emb"), lax.axis_index("seq")
    load = pltpu.make_async_copy(table_ref, table_v, load_sem)
    load.start()
    greet([(lax.rem(e + d, n_emb), s) for d in range(1, n_emb)]
          + [(e, lax.rem(s + d, n_seq)) for d in range(1, n_seq)])

    def ask(d):
        to = lax.rem(e + d, n_emb)
        return remote(req_ref.at[to], idx_ref.at[s, e], i_send.at[d], i_recv.at[d], to, s)

    for d in range(1, n_emb):
        ask(d).start()
    idx_ref[s, e] = req_ref[e]
    for d in range(1, n_emb):
        ask(d).wait_recv()

    def tell(d):
        to = lax.rem(s + d, n_seq)
        return remote(idx_ref.at[s], idx_ref.at[s], y_send.at[d], y_recv.at[d], e, to)

    for d in range(1, n_seq):
        tell(d).start()
    load.wait()
    shard = table_v.shape[0]
    lane = lax.broadcasted_iota(jnp.int32, (128, shard), 1)
    cap = tab_ref.shape[0] // n_emb
    per = 128 // cap
    groups = n_emb // per
    mine = e // per

    def answer(g, i, j):
        to = g * per + i
        src = rows_v.at[j, pl.ds(pl.multiple_of(i * cap, cap), cap)]
        dst = tab_ref.at[pl.ds(pl.multiple_of(e * cap, cap), cap)]
        return remote(src, dst, r_send.at[to], r_recv.at[e], to, s)

    for j in (2, 1, 3, 0):
        g = lax.rem(mine + j, groups)
        row = idx_ref[s, g * per]
        for i in range(1, per):
            row = row + idx_ref[s, g * per + i]
        col = jnp.transpose(jnp.broadcast_to(row, (8, 128)))[:, 0:1]
        hot = jnp.where(col == lane, 1.0, 0.0).astype(BF16)
        rows_v[j] = jnp.dot(hot, table_v[...], preferred_element_type=F32).astype(BF16)
        for t in range(per):
            i = lax.rem(lax.rem(e, per) + t, per)
            if j == 0 and t == 0:
                tab_ref[pl.ds(pl.multiple_of(e * cap, cap), cap), :] = rows_v[
                    0, pl.ds(pl.multiple_of(i * cap, cap), cap), :]
            else:
                answer(g, i, j).start()
    for d in range(1, n_emb):
        frm = lax.rem(e + d, n_emb)
        remote(rows_v.at[0, pl.ds(0, cap)], tab_ref.at[pl.ds(pl.multiple_of(frm * cap, cap), cap)],
               r_send.at[frm], r_recv.at[frm], frm, s).wait_recv()
    for d in range(1, n_seq):
        tell(d).wait()
    for d in range(1, n_emb):
        ask(d).wait_send()
        frm = lax.rem(e + d, n_emb)
        remote(rows_v.at[0, pl.ds(0, cap)], tab_ref.at[pl.ds(0, cap)],
               r_send.at[frm], r_recv.at[frm], frm, s).wait_send()


def fetch_rows_of(req, table, n_emb, n_seq, slots):
    vm = pl.BlockSpec(memory_space=pltpu.VMEM)
    width = table.shape[1]
    return pl.pallas_call(
        functools.partial(fetch, n_emb, n_seq),
        name="fetch",
        out_shape=(
            jax.ShapeDtypeStruct((slots, width), BF16),
            jax.ShapeDtypeStruct((n_seq, n_emb, 1, 128), jnp.int32),
        ),
        in_specs=[vm, pl.BlockSpec(memory_space=pl.ANY)],
        out_specs=(vm, vm),
        scratch_shapes=[
            pltpu.VMEM(table.shape, BF16),
            pltpu.VMEM((4, 128, width), BF16),
            pltpu.SemaphoreType.DMA,
            pltpu.SemaphoreType.DMA((n_emb,)),
            pltpu.SemaphoreType.DMA((n_emb,)),
            pltpu.SemaphoreType.DMA((n_seq,)),
            pltpu.SemaphoreType.DMA((n_seq,)),
            pltpu.SemaphoreType.DMA((n_emb,)),
            pltpu.SemaphoreType.DMA((n_emb,)),
        ],
        compiler_params=pltpu.CompilerParams(
            collective_id=0, has_side_effects=True, vmem_limit_bytes=40000000),
    )(req, table)


def share(n_emb, n_seq, sg_ref, g_ref, all_ref, sum_ref, half_s, pair_s, b1, p_s, b2, b3,
          g_send, g_recv, y_send, y_recv, z_send, z_recv, w_send, w_recv):
    e, s = lax.axis_index("emb"), lax.axis_index("seq")
    c, x, z = lax.rem(e, 2), lax.rem(e // 2, 4), e // 8
    cap = sg_ref.shape[0] // n_emb
    units = g_ref.shape[0]
    half, part, piece, bit = units // 2, units // 4, units // 16, units // 64
    along = {0: (x, z), 1: (z, x)}

    def peer(color, step, at):
        if (color + step) % 2 == 0:
            return (z * 4 + at) * 2 + c
        return (at * 4 + x) * 2 + c

    other = e + 1 - 2 * c
    greet([(lax.rem(e + d, n_emb), s) for d in range(1, n_emb)]
          + [(e, lax.rem(s + d, n_seq)) for d in range(1, n_seq)])

    def halve(k, j):
        src = g_ref.at[pl.ds((1 - c) * half + k * part + j * piece, piece)]
        return remote(src, pair_s.at[k, j], w_send.at[0, k, j], w_recv.at[0, k, j], other, s)

    def swap_grad(d):
        to = lax.rem(e + d, n_emb)
        return remote(sg_ref.at[pl.ds(pl.multiple_of(to * cap, cap), cap)],
                      all_ref.at[s, pl.ds(pl.multiple_of(e * cap, cap), cap)],
                      g_send.at[d], g_recv.at[d], to, s)

    for j in range(4):
        for k in range(2):
            halve(k, j).start()
    for d in range(1, n_emb):
        swap_grad(d).start()
    own = pl.ds(pl.multiple_of(e * cap, cap), cap)
    all_ref[s, own, :] = sg_ref[own, :]

    def spread(k, d):
        m = along[k][0]
        to = lax.rem(m + d, 4)
        return remote(half_s.at[k, to], b1.at[k, m], w_send.at[1, k, d], w_recv.at[1, k, d],
                      peer(k, 0, to), s)

    for j in range(4):
        for k in range(2):
            halve(k, j).wait_recv()
    for k in range(2):
        for d in (2, 1, 3, 0):
            j = lax.rem(along[k][0] + d, 4)
            mine = g_ref[pl.ds(c * half + k * part + j * piece, piece)].astype(F32)
            half_s[k, j] = (mine + pair_s[k, j].astype(F32)).astype(BF16)
            if d:
                spread(k, d).start()

    chunk = all_ref.shape[1] // 4
    up, down = lax.rem(s + 1, n_seq), lax.rem(s + n_seq - 1, n_seq)
    far = lax.rem(s + 2, n_seq)

    def pass_on(q, way):
        rows = pl.ds(q * chunk, chunk)
        return remote(all_ref.at[s, rows], all_ref.at[s, rows], y_send.at[way, q],
                      y_recv.at[way, q], e, down if way else up)

    def relay(q):
        frm, to = (down, up) if q < 2 else (up, down)
        rows = pl.ds(q * chunk, chunk)
        return remote(all_ref.at[frm, rows], all_ref.at[frm, rows], z_send.at[q], z_recv.at[q],
                      e, to)

    for d in range(1, n_emb):
        swap_grad(d).wait_recv()
    early = (0, 2)
    late = (1, 3)
    for q in early:
        for way in range(2):
            pass_on(q, way).start()

    def spread2(k, d):
        m = along[k][1]
        to = lax.rem(m + d, 4)
        return remote(p_s.at[k, to], b2.at[k, m], w_send.at[2, k, d], w_recv.at[2, k, d],
                      peer(k, 1, to), s)

    for k in range(2):
        m = along[k][0]
        total = half_s[k, m].astype(F32)
        for d in range(1, 4):
            spread(k, d).wait_recv()
        for d in range(1, 4):
            total = total + b1[k, lax.rem(m + d, 4)].astype(F32)
        for j in range(4):
            p_s[k, j] = total[j * bit : (j + 1) * bit].astype(BF16)
        for d in (2, 1, 3):
            spread2(k, d).start()

    def gather3(k, d):
        to = lax.rem(s + d, n_seq)
        return remote(b3.at[k, s], b3.at[k, s], w_send.at[3, k, d], w_recv.at[3, k, d], e, to)

    for k in range(2):
        m = along[k][1]
        total = p_s[k, m].astype(F32)
        for d in range(1, 4):
            spread2(k, d).wait_recv()
        for d in range(1, 4):
            total = total + b2[k, lax.rem(m + d, 4)].astype(F32)
        b3[k, s] = total.astype(BF16)
        for d in range(1, 4):
            gather3(k, d).start()
    for q in early:
        pass_on(q, 0 if q < 2 else 1).wait_recv()
        relay(q).start()
    for q in late:
        for way in range(2):
            pass_on(q, way).start()

    def place(k, first, second):
        return c * half + k * part + first * piece + second * bit

    def back2(k, d):
        to = lax.rem(along[k][1] + d, 4)
        ref = sum_ref.at[pl.ds(place(k, *along[k]), bit)]
        return remote(ref, ref, w_send.at[4, k, d], w_recv.at[4, k, d], peer(k, 1, to), s)

    def back1(k, d):
        to = lax.rem(along[k][0] + d, 4)
        ref = sum_ref.at[pl.ds(place(k, along[k][0], 0), piece)]
        return remote(ref, ref, w_send.at[5, k, d], w_recv.at[5, k, d], peer(k, 0, to), s)

    def back0(k, d):
        j = lax.rem(along[k][0] + 4 - d, 4)
        ref = sum_ref.at[pl.ds(place(k, j, 0), piece)]
        return remote(ref, ref, w_send.at[6, k, d], w_recv.at[6, k, d], other, s)

    for k in range(2):
        for d in range(1, 4):
            gather3(k, d).wait_recv()
        total = b3[k, 0].astype(F32)
        for j in range(1, 4):
            total = total + b3[k, j].astype(F32)
        sum_ref[pl.ds(place(k, *along[k]), bit)] = total.astype(BF16)
        for d in range(1, 4):
            back2(k, d).start()
    for k in range(2):
        for d in range(1, 4):
            back2(k, d).wait_recv()
        for d in (2, 1, 3):
            back1(k, d).start()
        back0(k, 0).start()
    for q in late:
        pass_on(q, 0 if q < 2 else 1).wait_recv()
        relay(q).start()
    for d in (1, 3, 2):
        for k in range(2):
            back1(k, d).wait_recv()
            back0(k, d).start()
    for q in range(4):
        pass_on(q, 1 if q < 2 else 0).wait_recv()
        relay(q).wait_recv()
    for k in range(2):
        for d in range(4):
            back0(k, d).wait_recv()

    for k in range(2):
        for j in range(4):
            halve(k, j).wait_send()
            back0(k, j).wait_send()
        for d in range(1, 4):
            for copy in (spread, spread2, gather3, back2, back1):
                copy(k, d).wait_send()
    for d in range(1, n_emb):
        swap_grad(d).wait_send()
    for q in range(4):
        relay(q).wait_send()
        for way in range(2):
            pass_on(q, way).wait_send()


def share_grads(sg, g, n_emb, n_seq):
    vm = pl.BlockSpec(memory_space=pltpu.VMEM)
    slots, width = sg.shape
    units = g.shape[0]
    tile = g.shape[1:]
    dma = pltpu.SemaphoreType.DMA
    return pl.pallas_call(
        functools.partial(share, n_emb, n_seq),
        name="share",
        out_shape=(
            jax.ShapeDtypeStruct((n_seq, slots, width), BF16),
            jax.ShapeDtypeStruct(g.shape, BF16),
        ),
        in_specs=[vm, vm],
        out_specs=(vm, vm),
        scratch_shapes=[
            pltpu.VMEM((2, 4, units // 16) + tile, BF16),
            pltpu.VMEM((2, 4, units // 16) + tile, BF16),
            pltpu.VMEM((2, 4, units // 16) + tile, BF16),
            pltpu.VMEM((2, 4, units // 64) + tile, BF16),
            pltpu.VMEM((2, 4, units // 64) + tile, BF16),
            pltpu.VMEM((2, n_seq, units // 64) + tile, BF16),
            dma((n_emb,)), dma((n_emb,)),
            dma((2, 4)), dma((2, 4)), dma((4,)), dma((4,)),
            dma((7, 2, 4)), dma((7, 2, 4)),
        ],
        compiler_params=pltpu.CompilerParams(
            collective_id=1, has_side_effects=True, vmem_limit_bytes=40000000),
    )(sg, g)


def finish(n_seq, idx_ref, all_ref, sum_ref, tg_ref, wi_ref, wo_ref, pick_s, tg_v, wi_v, wo_v, sems):
    s = lax.axis_index("seq")
    width = all_ref.shape[2]
    shard = tg_ref.shape[0]
    for b in range(16):
        wi_v[:, b * 128 : (b + 1) * 128] = sum_ref[b * 32 : (b + 1) * 32].reshape(width, 128).astype(F32)
    put_in = pltpu.make_async_copy(wi_v, wi_ref, sems.at[0])
    put_in.start()
    for b in range(4):
        wo_v[:, b * 128 : (b + 1) * 128] = (
            sum_ref[512 + b * 32 : 544 + b * 32].reshape(width, 128).astype(F32))
    put_out = pltpu.make_async_copy(wo_v, wo_ref, sems.at[1])
    put_out.start()
    sub = lax.broadcasted_iota(jnp.int32, (shard, 128), 0) + s * shard
    groups = idx_ref.shape[1] // 8
    for q in range(n_seq):
        for g in range(groups):
            row = idx_ref[q, 8 * g]
            for i in range(1, 8):
                row = row + idx_ref[q, 8 * g + i]
            at = (q * groups + g) * 128
            pick_s[:, at : at + 128] = jnp.where(sub == row, 1.0, 0.0).astype(BF16)
    cand = all_ref[...].reshape(-1, width)
    step = shard // 4
    copies = []
    for b in range(4):
        rows = slice(b * step, (b + 1) * step)
        tg_v[rows, :] = jnp.dot(pick_s[rows, :], cand, preferred_element_type=F32)
        copies.append(pltpu.make_async_copy(tg_v.at[rows], tg_ref.at[rows], sems.at[2 + b]))
        copies[-1].start()
    put_in.wait()
    put_out.wait()
    for copy in copies:
        copy.wait()


def finish_grads(idx, every, total, shard, width):
    vm = pl.BlockSpec(memory_space=pltpu.VMEM)
    hbm = pl.BlockSpec(memory_space=pl.ANY)
    n_seq = every.shape[0]
    return pl.pallas_call(
        functools.partial(finish, n_seq),
        name="finish",
        out_shape=(
            jax.ShapeDtypeStruct((shard, width), F32),
            jax.ShapeDtypeStruct((width, 4 * width), F32),
            jax.ShapeDtypeStruct((width, width), F32),
        ),
        in_specs=[vm, vm, vm],
        out_specs=(hbm, hbm, hbm),
        scratch_shapes=[
            pltpu.VMEM((shard, n_seq * every.shape[1]), BF16),
            pltpu.VMEM((shard, width), F32),
            pltpu.VMEM((width, 4 * width), F32),
            pltpu.VMEM((width, width), F32),
            pltpu.SemaphoreType.DMA((6,)),
        ],
        compiler_params=pltpu.CompilerParams(vmem_limit_bytes=50000000),
    )(idx, every, total)


def on_device(item_table, fetch_rows, event_slot, lengths, in_weight, out_weight, out_grad):
    n_emb, n_seq = lax.axis_size("emb"), lax.axis_size("seq")
    cap = fetch_rows.shape[-1]
    asked = fetch_rows.reshape(n_emb, cap)
    place = lax.broadcasted_iota(jnp.int32, (n_emb, 128), 1) // cap
    req = jnp.where(place == lax.rem(lax.axis_index("emb"), 128 // cap),
                    jnp.tile(asked, (1, 128 // cap)), 0)
    tab, idx = fetch_rows_of(req.reshape(n_emb, 1, 128), item_table, n_emb, n_seq, n_emb * cap)
    layer_out, slot_grad, weight_grad = local_layer(
        lengths, event_slot.reshape(-1, 128), tab, in_weight, out_weight, out_grad)
    every, total = share_grads(slot_grad, weight_grad, n_emb, n_seq)
    table_grad, in_total, out_total = finish_grads(
        idx, every, total, item_table.shape[0] // n_seq, item_table.shape[1])
    return layer_out, table_grad, in_total, out_total


def solution(mesh):
    both = P(("emb", "seq"))
    rows = P(("emb", "seq"), None)
    return jax.shard_map(
        on_device,
        mesh=mesh,
        in_specs=(P("emb", None), P("emb", "seq", None, None), both, rows, P(), P(), rows),
        out_specs=(rows, rows, P(), P()),
        check_vma=False,
    )
```

```python
import functools, math
import jax, jax.numpy as jnp
from jax import lax
from jax.experimental import pallas as pl
from jax.experimental.pallas import tpu as pltpu
from jax.sharding import PartitionSpec as P

F32, BF16 = jnp.float32, jnp.bfloat16
EPS = 1e-05
MOST = 512
B = 256
LAST = (((1,), (1,)), ((), ()))


def rows_at(i):
    return pl.ds(pl.multiple_of(i * B, B), B)


def expand(ev_ref, tab_ref, events_s, pick_s):
    slots = tab_ref.shape[0]
    ev = ev_ref[...]
    ev_t = jnp.transpose(ev)
    lane = lax.broadcasted_iota(jnp.int32, (128, slots), 1)
    sub = lax.broadcasted_iota(jnp.int32, (slots, 128), 0)
    for a in range(ev.shape[0]):
        hot = jnp.where(ev_t[:, a : a + 1] == lane, 1.0, 0.0).astype(BF16)
        events_s[128 * a : 128 * a + 128, :] = jnp.dot(
            hot, tab_ref[...], preferred_element_type=F32
        ).astype(BF16)
        pick_s[:, 128 * a : 128 * a + 128] = jnp.where(sub == ev[a : a + 1, :], 1.0, 0.0).astype(
            BF16
        )


def project(r, events_s, win_ref, normed_s, normed_t, rstd_s, gate_s, dsil_s, qkv_s, kv_t):
    rows = rows_at(r)
    width = events_s.shape[1]
    e = events_s[rows, :].astype(F32)
    c = e - jnp.mean(e, axis=-1, keepdims=True)
    rs = lax.rsqrt(jnp.mean(c * c, axis=-1, keepdims=True) + EPS)
    n = (c * rs).astype(BF16)
    normed_s[rows, :] = n
    rstd_s[rows, :] = rs
    normed_t[:, rows] = jnp.transpose(n)
    for b in range(4):
        cols = slice(b * width, (b + 1) * width)
        x = jnp.dot(n, win_ref[:, cols], preferred_element_type=F32)
        hx = 0.5 * x
        t = jnp.tanh(hx)
        u = 1.0 + t
        y = hx * u
        dsil_s[rows, cols] = (0.5 * (u + hx * (1.0 - t * t))).astype(BF16)
        if b == 0:
            gate_s[rows, :] = y
        else:
            yb = y.astype(BF16)
            qkv_s[b - 1, rows, :] = yb
            if b == 1:
                kv_t[1, :, rows] = jnp.transpose(yb)
            elif b == 3:
                kv_t[0, :, rows] = jnp.transpose(yb)


def pairs(blocks):
    back = MOST // B
    return [(q, k) for q in range(blocks) for k in range(max(0, q - back), q + 1)]


def attend(h, starts, qkv_s, kv_t, att_t, p_s, d_s, blocks):
    hc = pl.ds(pl.multiple_of(h * 128, 128), 128)
    lane = lax.broadcasted_iota(jnp.int32, (B, B), 1)
    sub = lax.broadcasted_iota(jnp.int32, (B, B), 0)
    head = 128
    c1 = 0.5 / math.sqrt(head)
    total = None
    for i, (q, k) in enumerate(pairs(blocks)):
        kk = qkv_s[2, k * B : (k + 1) * B, hc]
        qq = qkv_s[1, q * B : (q + 1) * B, hc]
        x = lax.dot_general(kk, qq, LAST, preferred_element_type=F32)
        hh = x * c1
        t = jnp.tanh(hh)
        u = 1.0 + t
        mask = (sub + k * B) >= starts[q]
        if q == k:
            mask = mask & (sub <= lane)
        w = jnp.where(mask, (hh * u) * (1.0 / MOST), 0.0).astype(BF16)
        d = jnp.where(mask, (u + hh * (1.0 - t * t)) * (c1 / MOST), 0.0).astype(BF16)
        p_s[h, i] = w
        d_s[h, i] = d
        o = jnp.dot(kv_t[1, hc, k * B : (k + 1) * B], w, preferred_element_type=F32)
        total = o if k == max(0, q - MOST // B) else total + o
        if q == k:
            att_t[hc, q * B : (q + 1) * B] = total


def middle(r, att_t, gate_s, dsil_s, events_s, wout_ref, og_ref, lo_ref, gated_t, dx_s, do_s):
    rows = rows_at(r)
    width = events_s.shape[1]
    a = jnp.transpose(att_t[:, rows])
    c = a - jnp.mean(a, axis=-1, keepdims=True)
    rs = lax.rsqrt(jnp.mean(c * c, axis=-1, keepdims=True) + EPS)
    xh = c * rs
    gate = gate_s[rows, :]
    gated = (xh * gate).astype(BF16)
    out = jnp.dot(gated, wout_ref[...], preferred_element_type=F32)
    lo_ref[rows, :] = (out + events_s[rows, :].astype(F32)).astype(BF16)
    gated_t[:, rows] = jnp.transpose(gated)
    og = og_ref[rows, :]
    dg = lax.dot_general(og, wout_ref[...], LAST, preferred_element_type=F32)
    dg = dg.astype(BF16).astype(F32)
    dx_s[rows, :width] = (dg * xh * dsil_s[rows, :width].astype(F32)).astype(BF16)
    dxh = dg * gate
    m1 = jnp.mean(dxh, axis=-1, keepdims=True)
    m2 = jnp.mean(dxh * xh, axis=-1, keepdims=True)
    do_s[rows, :] = (rs * (dxh - m1 - xh * m2)).astype(BF16)


def attend_back(h, qkv_s, kv_t, p_s, d_s, do_s, dsil_s, dx_s, dq_t, blocks, width):
    hc = slice(h * 128, (h + 1) * 128)

    def put(block, part, grad):
        cols = slice(part * width + h * 128, part * width + (h + 1) * 128)
        rows = slice(block * B, (block + 1) * B)
        dx_s[rows, cols] = (
            grad.astype(BF16).astype(F32) * dsil_s[rows, cols].astype(F32)
        ).astype(BF16)

    order = pairs(blocks)
    for k in range(blocks):
        dv = dk = None
        vv = qkv_s[0, k * B : (k + 1) * B, hc]
        for q in range(k, min(k + MOST // B, blocks - 1) + 1):
            i = order.index((q, k))
            do = do_s[q * B : (q + 1) * B, hc]
            dp = lax.dot_general(vv, do, LAST, preferred_element_type=F32).astype(BF16)
            ds = dp * d_s[h, i]
            dv1 = jnp.dot(p_s[h, i], do, preferred_element_type=F32)
            dk1 = jnp.dot(ds, qkv_s[1, q * B : (q + 1) * B, hc], preferred_element_type=F32)
            dv = dv1 if dv is None else dv + dv1
            dk = dk1 if dk is None else dk + dk1
            dq1 = jnp.dot(kv_t[0, hc, k * B : (k + 1) * B], ds, preferred_element_type=F32)
            at = slice(q * B, (q + 1) * B)
            if k == max(0, q - MOST // B):
                dq_t[:, at] = dq1
            else:
                dq_t[:, at] += dq1
        put(k, 1, dv)
        put(k, 3, dk)
    for q in range(blocks):
        put(q, 2, jnp.transpose(dq_t[:, q * B : (q + 1) * B]))


def event_back(r, dx_s, win_ref, normed_s, rstd_s, og_ref, eg_s):
    rows = rows_at(r)
    g = lax.dot_general(dx_s[rows, :], win_ref[...], LAST, preferred_element_type=F32)
    g = g.astype(BF16).astype(F32)
    xh = normed_s[rows, :].astype(F32)
    m1 = jnp.mean(g, axis=-1, keepdims=True)
    m2 = jnp.mean(g * xh, axis=-1, keepdims=True)
    de = (rstd_s[rows, :] * (g - m1 - xh * m2)).astype(BF16)
    eg_s[rows, :] = (de.astype(F32) + og_ref[rows, :].astype(F32)).astype(BF16)


def row_starts(len_ref, blocks):
    ends, at = [], jnp.int32(0)
    for s in range(len_ref.shape[1]):
        at = at + len_ref[0, s]
        ends.append(at)
    starts = []
    for q in range(blocks):
        place = lax.broadcasted_iota(jnp.int32, (1, B), 1) + q * B
        start = jnp.zeros((1, B), jnp.int32)
        for e in ends:
            start = jnp.where(place >= e, e, start)
        starts.append(start)
    return starts


def compute_scratch(tokens, width, slots):
    n = len(pairs(tokens // B))
    heads = width // 128
    return [
        pltpu.VMEM((tokens, width), BF16),
        pltpu.VMEM((slots, tokens), BF16),
        pltpu.VMEM((tokens, width), BF16),
        pltpu.VMEM((width, tokens), BF16),
        pltpu.VMEM((tokens, 1), F32),
        pltpu.VMEM((tokens, width), F32),
        pltpu.VMEM((tokens, 4 * width), BF16),
        pltpu.VMEM((3, tokens, width), BF16),
        pltpu.VMEM((2, width, tokens), BF16),
        pltpu.VMEM((width, tokens), F32),
        pltpu.VMEM((heads, n, B, B), BF16),
        pltpu.VMEM((heads, n, B, B), BF16),
        pltpu.VMEM((width, tokens), BF16),
        pltpu.VMEM((tokens, 4 * width), BF16),
        pltpu.VMEM((tokens, width), BF16),
        pltpu.VMEM((128, tokens), F32),
        pltpu.VMEM((tokens, width), BF16),
    ]


MESH = pl.DeviceIdType.MESH


def remote(src, dst, send_sem, recv_sem, emb, seq):
    return pltpu.make_async_remote_copy(
        src_ref=src, dst_ref=dst, send_sem=send_sem, recv_sem=recv_sem,
        device_id=(emb, seq), device_id_type=MESH,
    )


def rows_of(at, count):
    return pl.ds(pl.multiple_of(at * count, count), count)


def greet(peers):
    barrier = pltpu.get_barrier_semaphore()
    for emb, seq in peers:
        pl.semaphore_signal(barrier, inc=1, device_id=(emb, seq), device_id_type=MESH)
    pl.semaphore_wait(barrier, len(peers))


class Summed:
    def __init__(self, e, s, base, units, g_s, sum_s, bufs, sems):
        self.e, self.s = e, s
        self.c, self.x, self.z = lax.rem(e, 2), lax.rem(e // 2, 4), e // 8
        self.chip = e // 2
        self.other = e + 1 - 2 * self.c
        self.base, self.half, self.piece = base, units // 2, units // 32
        self.g_s, self.sum_s = g_s, sum_s
        self.half_s, self.pair_s, self.b1, self.b3 = bufs
        self.many_send, self.many_recv, self.few_send, self.few_recv = sems

    def chips(self, t):
        z = lax.rem(self.z + t, 4)
        return [z * 4 + lax.rem(self.x + u, 4) for u in range(0 if t else 1, 4)]

    def line(self, t):
        return lax.rem(self.z + t, 4) * 4 * self.piece

    def halve(self, t):
        src = self.g_s.at[pl.ds(self.base + (1 - self.c) * self.half + self.line(t), 4 * self.piece)]
        dst = self.pair_s.at[pl.ds(self.line(t), 4 * self.piece)]
        return remote(src, dst, self.few_send.at[0, t], self.few_recv.at[0, t], self.other, self.s)

    def spread(self, to):
        return remote(self.half_s.at[pl.ds(to * self.piece, self.piece)], self.b1.at[self.chip],
                      self.many_send.at[0, to], self.many_recv.at[0, self.chip],
                      to * 2 + self.c, self.s)

    def spread_from(self, frm):
        return remote(self.half_s.at[pl.ds(0, self.piece)], self.b1.at[frm],
                      self.many_send.at[0, frm], self.many_recv.at[0, frm],
                      frm * 2 + self.c, self.s)

    def gather3(self, d):
        ref = self.b3.at[self.s]
        return remote(ref, ref, self.few_send.at[1, d], self.few_recv.at[1, d],
                      self.e, lax.rem(self.s + d, 4))

    def own(self, chip):
        return self.sum_s.at[pl.ds(self.base + self.c * self.half + chip * self.piece, self.piece)]

    def back(self, to):
        return remote(self.own(self.chip), self.own(self.chip),
                      self.many_send.at[1, to], self.many_recv.at[1, self.chip],
                      to * 2 + self.c, self.s)

    def back_from(self, frm):
        return remote(self.own(frm), self.own(frm),
                      self.many_send.at[1, frm], self.many_recv.at[1, frm],
                      frm * 2 + self.c, self.s)

    def join(self, t):
        ref = self.sum_s.at[pl.ds(self.base + self.c * self.half + self.line(t), 4 * self.piece)]
        return remote(ref, ref, self.few_send.at[2, t], self.few_recv.at[2, t], self.other, self.s)

    def step0(self):
        for t in (2, 1, 3, 0):
            self.halve(t).start()

    def step1(self):
        for t in (2, 1, 3, 0):
            self.halve(t).wait_recv()
            part = pl.ds(self.line(t), 4 * self.piece)
            mine = self.g_s[pl.ds(self.base + self.c * self.half + self.line(t), 4 * self.piece)]
            self.half_s[part] = (mine.astype(F32) + self.pair_s[part].astype(F32)).astype(BF16)
            for to in self.chips(t):
                self.spread(to).start()

    def step2(self):
        total = self.half_s[pl.ds(self.chip * self.piece, self.piece)].astype(F32)
        for t in range(4):
            for frm in self.chips(t):
                self.spread_from(frm).wait_recv()
        for t in range(4):
            for frm in self.chips(t):
                total = total + self.b1[frm].astype(F32)
        self.b3[self.s] = total.astype(BF16)
        for d in (2, 1, 3):
            self.gather3(d).start()

    def step3(self):
        for d in range(1, 4):
            self.gather3(d).wait_recv()
        total = self.b3[0].astype(F32)
        for j in range(1, 4):
            total = total + self.b3[j].astype(F32)
        self.own(self.chip)[...] = total.astype(BF16)
        for t in (2, 1, 3, 0):
            for to in self.chips(t):
                self.back(to).start()

    def step4(self):
        for t in (0, 1, 3, 2):
            for frm in self.chips(t):
                self.back_from(frm).wait_recv()
            self.join(t).start()

    def step5(self):
        for t in range(4):
            self.join(t).wait_recv()

    def drain(self):
        for t in range(4):
            self.halve(t).wait_send()
            self.join(t).wait_send()
            for to in self.chips(t):
                self.spread(to).wait_send()
                self.back(to).wait_send()
        for d in range(1, 4):
            self.gather3(d).wait_send()


PARTS = (256, 192, 192)


def whole(n_emb, n_seq, len_ref, asked_ref, ev_ref, table_ref, win_ref, wout_ref, og_ref,
          lo_ref, tg_ref, total_ref,
          idx_ref, tgb_s, req_ref, table_v, rows_v, tab_s, win_s, wout_s, og_s, lo_s, g_s, sum_s, sg_s, all_s,
          bufs_e, bufs_m, bufs_l, load, save, i_send, i_recv, j_send, j_recv, r_send, r_recv, g_send, g_recv,
          y_send, y_recv, z_send, z_recv, many_send, many_recv, few_send, few_recv,
          events_s, pick_s, normed_s, normed_t, rstd_s, gate_s, dsil_s, qkv_s, kv_t,
          att_t, p_s, d_s, gated_t, dx_s, do_s, dq_t, eg_s):
    e, s = lax.axis_index("emb"), lax.axis_index("seq")
    tokens, width = og_s.shape
    blocks, heads = tokens // B, width // 128
    cap = tab_s.shape[0] // n_emb
    per = 128 // cap
    groups = n_emb // per
    mine, inner = e // per, lax.rem(e, per)
    loads = [pltpu.make_async_copy(a, b, load.at[i]) for i, (a, b) in enumerate(
        ((table_ref, table_v), (win_ref, win_s), (og_ref, og_s), (wout_ref, wout_s)))]
    for copy in loads:
        copy.start()
    greet([(lax.rem(e + d, n_emb), s) for d in range(1, n_emb)]
          + [(e, lax.rem(s + d, n_seq)) for d in range(1, n_seq)])

    def members(j):
        g = lax.rem(mine + j, groups)
        first = 1 if j == 0 else 0
        return g, [g * per + lax.rem(inner + t, per) for t in range(first, per)]

    def ask(to):
        return remote(req_ref.at[to], idx_ref.at[s, e], i_send.at[to], i_recv.at[e], to, s)

    def asked(frm):
        return remote(req_ref.at[frm], idx_ref.at[s, frm], i_send.at[frm], i_recv.at[frm], frm, s)

    rows_asked = asked_ref[0, 0]
    spot = jnp.where(lax.broadcasted_iota(jnp.int32, (cap, 128), 1)
                     == lax.broadcasted_iota(jnp.int32, (cap, 128), 0) + cap * inner, 1.0, 0.0)
    low = rows_asked & 127
    high = (rows_asked - low).astype(F32)
    spread_out = (jnp.dot(high.astype(BF16), spot.astype(BF16), preferred_element_type=F32)
                  + jnp.dot(low.astype(F32).astype(BF16), spot.astype(BF16),
                            preferred_element_type=F32)).astype(jnp.int32)
    for to in range(n_emb):
        req_ref[to] = spread_out[to : to + 1, :]
    for j in (2, 1, 3, 0):
        for to in members(j)[1]:
            ask(to).start()
    idx_ref[s, e] = req_ref[e]
    shard = table_v.shape[0]
    lane = lax.broadcasted_iota(jnp.int32, (128, shard), 1)

    def answer(to, j):
        return remote(rows_v.at[j, rows_of(lax.rem(to, per), cap)], tab_s.at[rows_of(e, cap)],
                      r_send.at[to], r_recv.at[e], to, s)

    def answered(frm, j):
        return remote(rows_v.at[j, rows_of(lax.rem(frm, per), cap)], tab_s.at[rows_of(frm, cap)],
                      r_send.at[frm], r_recv.at[frm], frm, s)

    loads[0].wait()
    for j in (0, 1, 3, 2):
        g, them = members(j)
        for frm in them:
            asked(frm).wait_recv()
        row = idx_ref[s, g * per]
        for i in range(1, per):
            row = row + idx_ref[s, g * per + i]
        col = jnp.transpose(jnp.broadcast_to(row, (8, 128)))[:, 0:1]
        hot = jnp.where(col == lane, 1.0, 0.0).astype(BF16)
        rows_v[j] = jnp.dot(hot, table_v[...], preferred_element_type=F32).astype(BF16)
        for to in them:
            answer(to, j).start()
        if j == 0:
            tab_s[rows_of(e, cap), :] = rows_v[0, rows_of(inner, cap), :]

    def tell(d):
        to = lax.rem(s + d, n_seq)
        return remote(idx_ref.at[s], idx_ref.at[s], j_send.at[d], j_recv.at[d], e, to)

    for d in range(1, n_seq):
        tell(d).start()
    for j in range(groups):
        for frm in members(j)[1]:
            answered(frm, j).wait_recv()
    for copy in loads[1:]:
        copy.wait()

    expand(ev_ref, tab_s, events_s, pick_s)
    pl.loop(0, blocks)(lambda r: project(
        r, events_s, win_s, normed_s, normed_t, rstd_s, gate_s, dsil_s, qkv_s, kv_t))
    starts = row_starts(len_ref, blocks)
    pl.loop(0, heads)(lambda h: attend(h, starts, qkv_s, kv_t, att_t, p_s, d_s, blocks))
    pl.loop(0, blocks)(lambda r: middle(
        r, att_t, gate_s, dsil_s, events_s, wout_s, og_s, lo_s, gated_t, dx_s, do_s))
    saves = [pltpu.make_async_copy(lo_s, lo_ref, save.at[0])]
    saves[0].start()

    def put_grad(c, val):
        g_s[pl.ds(c * 64, 32)] = val[:, :128].astype(BF16).reshape(32, 16, 128)
        g_s[pl.ds(c * 64 + 32, 32)] = val[:, 128:].astype(BF16).reshape(32, 16, 128)

    for c in range(2):
        put_grad(c, jnp.dot(normed_t[...], dx_s[:, c * B : (c + 1) * B],
                            preferred_element_type=F32))
        put_grad(2 + c, jnp.dot(gated_t[...], og_s[:, c * B : (c + 1) * B],
                                preferred_element_type=F32))
    sums, base = [], 0
    for i, (units, bufs) in enumerate(zip(PARTS, (bufs_e, bufs_m, bufs_l))):
        sems = [sem.at[i] for sem in (many_send, many_recv, few_send, few_recv)]
        sums.append(Summed(e, s, base, units, g_s, sum_s, bufs, sems))
        base += units
    early, mid, late = sums
    early.step0()

    def back(h):
        attend_back(h, qkv_s, kv_t, p_s, d_s, do_s, dsil_s, dx_s, dq_t, blocks, width)

    def grads_of(c):
        for b in range(3):
            cols = slice((b + 1) * width + c * B, (b + 1) * width + (c + 1) * B)
            put_grad(4 + 3 * c + b, jnp.dot(normed_t[...], dx_s[:, cols],
                                            preferred_element_type=F32))

    back(0)
    early.step1()
    back(1)
    grads_of(0)
    mid.step0()
    back(2)
    mid.step1()
    back(3)
    early.step2()
    pl.loop(0, blocks)(lambda r: event_back(r, dx_s, win_s, normed_s, rstd_s, og_s, eg_s))
    early.step3()
    sg_s[...] = jnp.dot(pick_s[...], eg_s[...], preferred_element_type=F32).astype(BF16)

    def give(to):
        return remote(sg_s.at[rows_of(to, cap)], all_s.at[s, rows_of(e, cap)],
                      g_send.at[to], g_recv.at[e], to, s)

    def given(frm):
        return remote(sg_s.at[rows_of(frm, cap)], all_s.at[s, rows_of(frm, cap)],
                      g_send.at[frm], g_recv.at[frm], frm, s)

    for j in (0, 1, 3, 2):
        for to in members(j)[1]:
            give(to).start()
    all_s[s, rows_of(e, cap), :] = sg_s[rows_of(e, cap), :]
    grads_of(1)
    late.step0()
    mid.step2()
    chunk = all_s.shape[1] // groups
    up, down = lax.rem(s + 1, n_seq), lax.rem(s + n_seq - 1, n_seq)

    def pass_on(j, way):
        ref = all_s.at[s, rows_of(lax.rem(mine + j, groups), chunk)]
        return remote(ref, ref, y_send.at[way, j], y_recv.at[way, j], e, down if way else up)

    def relay(j):
        frm, to = (down, up) if j % 2 else (up, down)
        ref = all_s.at[frm, rows_of(lax.rem(mine + j, groups), chunk)]
        return remote(ref, ref, z_send.at[j], z_recv.at[j], e, to)

    def arrived(j):
        for frm in members(j)[1]:
            given(frm).wait_recv()
        for way in range(2):
            pass_on(j, way).start()

    def further(j):
        pass_on(j, 0 if j % 2 else 1).wait_recv()
        relay(j).start()

    def keep(i):
        rows = pl.ds(sums[i].base, PARTS[i])
        saves.append(pltpu.make_async_copy(sum_s.at[rows], total_ref.at[rows], save.at[2 + i]))
        saves[-1].start()

    part = gate_s.shape[0]
    sub = lax.broadcasted_iota(jnp.int32, (part, 128), 0) + s * part
    for d in range(1, n_seq):
        tell(d).wait_recv()
    for n in range(n_seq):
        for j in range(groups):
            g = lax.rem(mine + j, groups)
            frm = lax.rem(s + n, n_seq)
            row = idx_ref[frm, g * per]
            for i in range(1, per):
                row = row + idx_ref[frm, g * per + i]
            at = (n * groups + j) * 128
            dsil_s[:, at : at + 128] = jnp.where(sub == row, 1.0, 0.0).astype(BF16)

    def add(n, js):
        frm = lax.rem(s + n, n_seq)
        rows = jnp.concatenate(
            [all_s[frm, rows_of(lax.rem(mine + j, groups), chunk), :] for j in js], axis=0)
        at = (n * groups + js[0]) * 128

        @pl.loop(0, blocks)
        def _(r):
            val = jnp.dot(dsil_s[rows_at(r), at : at + 256], rows, preferred_element_type=F32)
            if n == 0 and js[0] == 0:
                gate_s[rows_at(r), :] = val
            else:
                gate_s[rows_at(r), :] += val

    def keep(i):
        rows = pl.ds(sums[i].base, PARTS[i])
        saves.append(pltpu.make_async_copy(sum_s.at[rows], total_ref.at[rows], save.at[2 + i]))
        saves[-1].start()

    arrived(0)
    late.step1()
    arrived(1)
    mid.step3()
    early.step4()
    further(0)
    add(0, (0, 1))
    arrived(2)
    late.step2()
    further(1)
    arrived(3)
    mid.step4()
    add(0, (2, 3))
    late.step3()
    further(2)
    early.step5()
    keep(0)
    for way in range(2):
        for j in (0, 1):
            if way != (0 if j % 2 else 1):
                pass_on(j, way).wait_recv()
    add(1, (0, 1))
    add(3, (0, 1))
    further(3)
    mid.step5()
    keep(1)
    late.step4()
    for way in range(2):
        for j in (2, 3):
            if way != (0 if j % 2 else 1):
                pass_on(j, way).wait_recv()
    add(1, (2, 3))
    add(3, (2, 3))
    relay(0).wait_recv()
    relay(1).wait_recv()
    add(2, (0, 1))
    late.step5()
    keep(2)
    relay(2).wait_recv()
    relay(3).wait_recv()
    add(2, (2, 3))
    tgb_s[...] = gate_s[...].astype(BF16)
    saves.append(pltpu.make_async_copy(tgb_s, tg_ref, save.at[1]))
    saves[-1].start()
    for d in range(1, n_seq):
        tell(d).wait_send()
    for j in range(groups):
        for to in members(j)[1]:
            ask(to).wait_send()
            answer(to, j).wait_send()
            give(to).wait_send()
        relay(j).wait_send()
        for way in range(2):
            pass_on(j, way).wait_send()
    for part in sums:
        part.drain()
    for copy in saves:
        copy.wait()


def layer_grads(lengths, asked, ev, table, win, wout, og, n_emb, n_seq, slots):
    vm = pl.BlockSpec(memory_space=pltpu.VMEM)
    hbm = pl.BlockSpec(memory_space=pl.ANY)
    tokens, width = og.shape
    tile = (16, 128)
    units = 5 * width * width // (16 * 128)
    dma = pltpu.SemaphoreType.DMA

    def sums(n):
        shapes = [(n // 2,), (n // 2,), (16, n // 32), (n_seq, n // 32)]
        return tuple(pltpu.VMEM(shape + tile, BF16) for shape in shapes)

    return pl.pallas_call(
        functools.partial(whole, n_emb, n_seq),
        name="layer",
        out_shape=(
            jax.ShapeDtypeStruct((tokens, width), BF16),
            jax.ShapeDtypeStruct((tokens, width), BF16),
            jax.ShapeDtypeStruct((units,) + tile, BF16),
        ),
        in_specs=[pl.BlockSpec(memory_space=pltpu.SMEM), vm, vm] + [hbm] * 4,
        out_specs=(hbm, hbm, hbm),
        scratch_shapes=[
            pltpu.VMEM((n_seq, n_emb, 1, 128), jnp.int32),
            pltpu.VMEM((tokens, width), BF16),
            pltpu.VMEM((n_emb, 1, 128), jnp.int32),
            pltpu.VMEM(table.shape, BF16),
            pltpu.VMEM((4, 128, width), BF16),
            pltpu.VMEM((slots, width), BF16),
            pltpu.VMEM(win.shape, BF16),
            pltpu.VMEM(wout.shape, BF16),
            pltpu.VMEM(og.shape, BF16),
            pltpu.VMEM(og.shape, BF16),
            pltpu.VMEM((units,) + tile, BF16),
            pltpu.VMEM((units,) + tile, BF16),
            pltpu.VMEM((slots, width), BF16),
            pltpu.VMEM((n_seq, slots, width), BF16),
        ] + [sums(n) for n in PARTS] + [
            dma((4,)), dma((5,)),
            dma((n_emb,)), dma((n_emb,)), dma((n_seq,)), dma((n_seq,)),
            dma((n_emb,)), dma((n_emb,)), dma((n_emb,)), dma((n_emb,)),
            dma((2, 4)), dma((2, 4)), dma((4,)), dma((4,)),
            dma((3, 2, 16)), dma((3, 2, 16)), dma((3, 3, 4)), dma((3, 3, 4)),
        ] + compute_scratch(tokens, width, slots),
        compiler_params=pltpu.CompilerParams(
            collective_id=0, has_side_effects=True, vmem_limit_bytes=67043328),
    )(lengths, asked, ev, table, win, wout, og)


def finish(rows_ref, sum_ref, out_ref, tg_ref, wi_ref, wo_ref, lo_ref,
           rows_s, sum_s, lo_s, tg_v, wi_v, wo_v, load, sems):
    width = lo_s.shape[1]
    loads = [pltpu.make_async_copy(a, b, load.at[i]) for i, (a, b) in enumerate(
        ((rows_ref, rows_s), (sum_ref, sum_s), (out_ref, lo_s)))]
    for copy in loads:
        copy.start()
    loads[0].wait()
    tg_v[...] = rows_s[...].astype(F32)
    copies = [pltpu.make_async_copy(tg_v, tg_ref, sems.at[6])]
    copies[-1].start()
    loads[1].wait()
    tall = width // 4
    for r in range(4):
        for b in range(20):
            val = sum_s[b * 32 + r * 8 : b * 32 + r * 8 + 8].reshape(tall, 128).astype(F32)
            rows = slice(r * tall, (r + 1) * tall)
            if 4 <= b < 8:
                wo_v[rows, (b - 4) * 128 : (b - 3) * 128] = val
            else:
                half, part, head = (b - 8) // 6, (b - 8) % 6 // 2, b % 2
                at = b if b < 4 else 4 + part * 4 + half * 2 + head
                wi_v[rows, at * 128 : (at + 1) * 128] = val
        copies.append(pltpu.make_async_copy(wi_v.at[rows], wi_ref.at[rows], sems.at[r]))
        copies[-1].start()
    copies.append(pltpu.make_async_copy(wo_v, wo_ref, sems.at[4]))
    copies[-1].start()
    loads[2].wait()
    copies.append(pltpu.make_async_copy(lo_s, lo_ref, sems.at[5]))
    copies[-1].start()
    for copy in copies:
        copy.wait()


def finish_grads(rows, total, out):
    hbm = pl.BlockSpec(memory_space=pl.ANY)
    width = out.shape[1]
    shapes = [(rows.shape, F32), ((width, 4 * width), F32), ((width, width), F32)]
    return pl.pallas_call(
        finish,
        name="finish",
        out_shape=tuple(jax.ShapeDtypeStruct(*a) for a in shapes + [(out.shape, BF16)]),
        in_specs=[hbm] * 3,
        out_specs=(hbm,) * 4,
        scratch_shapes=[pltpu.VMEM(a.shape, BF16) for a in (rows, total, out)]
        + [pltpu.VMEM(*a) for a in shapes]
        + [pltpu.SemaphoreType.DMA((3,)), pltpu.SemaphoreType.DMA((7,))],
        compiler_params=pltpu.CompilerParams(vmem_limit_bytes=67043328),
    )(rows, total, out)


def on_device(item_table, fetch_rows, event_slot, lengths, in_weight, out_weight, out_grad):
    n_emb, n_seq = lax.axis_size("emb"), lax.axis_size("seq")
    cap = fetch_rows.shape[-1]
    layer_out, rows_grad, total = layer_grads(
        lengths, fetch_rows, event_slot.reshape(-1, 128), item_table,
        in_weight, out_weight, out_grad, n_emb, n_seq, n_emb * cap)
    table_grad, in_total, out_total, layer_out = finish_grads(rows_grad, total, layer_out)
    return layer_out, table_grad, in_total, out_total


def solution(mesh):
    both = P(("emb", "seq"))
    rows = P(("emb", "seq"), None)
    return jax.shard_map(
        on_device,
        mesh=mesh,
        in_specs=(P("emb", None), P("emb", "seq", None, None), both, rows, P(), P(), rows),
        out_specs=(rows, rows, P(), P()),
        check_vma=False,
    )
```

```python
import functools, math
import jax, jax.numpy as jnp
from jax import lax
from jax.experimental import pallas as pl
from jax.experimental.pallas import tpu as pltpu
from jax.sharding import PartitionSpec as P

F32, BF16 = jnp.float32, jnp.bfloat16
EPS = 1e-05
MOST = 512
B = 256
LAST = (((1,), (1,)), ((), ()))


def rows_at(i):
    return pl.ds(pl.multiple_of(i * B, B), B)


def expand(ev_ref, tab_ref, events_s, pick_s):
    slots = tab_ref.shape[0]
    ev = ev_ref[...]
    ev_t = jnp.transpose(ev)
    lane = lax.broadcasted_iota(jnp.int32, (128, slots), 1)
    sub = lax.broadcasted_iota(jnp.int32, (slots, 128), 0)
    for a in range(ev.shape[0]):
        hot = jnp.where(ev_t[:, a : a + 1] == lane, 1.0, 0.0).astype(BF16)
        events_s[128 * a : 128 * a + 128, :] = jnp.dot(
            hot, tab_ref[...], preferred_element_type=F32
        ).astype(BF16)
        pick_s[:, 128 * a : 128 * a + 128] = jnp.where(sub == ev[a : a + 1, :], 1.0, 0.0).astype(
            BF16
        )


def project(r, events_s, win_ref, normed_s, normed_t, rstd_s, gate_s, dsil_s, qkv_s, kv_t):
    rows = rows_at(r)
    width = events_s.shape[1]
    e = events_s[rows, :].astype(F32)
    c = e - jnp.mean(e, axis=-1, keepdims=True)
    rs = lax.rsqrt(jnp.mean(c * c, axis=-1, keepdims=True) + EPS)
    n = (c * rs).astype(BF16)
    normed_s[rows, :] = n
    rstd_s[rows, :] = rs
    normed_t[:, rows] = jnp.transpose(n)
    for b in range(4):
        cols = slice(b * width, (b + 1) * width)
        x = jnp.dot(n, win_ref[:, cols], preferred_element_type=F32)
        hx = 0.5 * x
        t = jnp.tanh(hx)
        u = 1.0 + t
        y = hx * u
        dsil_s[rows, cols] = (0.5 * (u + hx * (1.0 - t * t))).astype(BF16)
        if b == 0:
            gate_s[rows, :] = y
        else:
            yb = y.astype(BF16)
            qkv_s[b - 1, rows, :] = yb
            if b == 1:
                kv_t[1, :, rows] = jnp.transpose(yb)
            elif b == 3:
                kv_t[0, :, rows] = jnp.transpose(yb)


def pairs(blocks):
    back = MOST // B
    return [(q, k) for q in range(blocks) for k in range(max(0, q - back), q + 1)]


def attend(h, starts, qkv_s, kv_t, att_t, p_s, d_s, blocks):
    hc = pl.ds(pl.multiple_of(h * 128, 128), 128)
    lane = lax.broadcasted_iota(jnp.int32, (B, B), 1)
    sub = lax.broadcasted_iota(jnp.int32, (B, B), 0)
    head = 128
    c1 = 0.5 / math.sqrt(head)
    total = None
    for i, (q, k) in enumerate(pairs(blocks)):
        kk = qkv_s[2, k * B : (k + 1) * B, hc]
        qq = qkv_s[1, q * B : (q + 1) * B, hc]
        x = lax.dot_general(kk, qq, LAST, preferred_element_type=F32)
        hh = x * c1
        t = jnp.tanh(hh)
        u = 1.0 + t
        mask = (sub + k * B) >= starts[q]
        if q == k:
            mask = mask & (sub <= lane)
        w = jnp.where(mask, hh * u, 0.0).astype(BF16)
        d = jnp.where(mask, u + hh * (1.0 - t * t), 0.0).astype(BF16)
        p_s[h, i] = w
        d_s[h, i] = d
        o = jnp.dot(kv_t[1, hc, k * B : (k + 1) * B], w, preferred_element_type=F32)
        total = o if k == max(0, q - MOST // B) else total + o
        if q == k:
            att_t[hc, q * B : (q + 1) * B] = total * (1.0 / MOST)


def middle(r, att_t, gate_s, dsil_s, events_s, wout_ref, og_ref, lo_ref, gated_t, dx_s, do_s):
    rows = rows_at(r)
    width = events_s.shape[1]
    a = jnp.transpose(att_t[:, rows])
    c = a - jnp.mean(a, axis=-1, keepdims=True)
    rs = lax.rsqrt(jnp.mean(c * c, axis=-1, keepdims=True) + EPS)
    xh = c * rs
    gate = gate_s[rows, :]
    gated = (xh * gate).astype(BF16)
    out = jnp.dot(gated, wout_ref[...], preferred_element_type=F32)
    lo_ref[rows, :] = (out + events_s[rows, :].astype(F32)).astype(BF16)
    gated_t[:, rows] = jnp.transpose(gated)
    og = og_ref[rows, :]
    dg = lax.dot_general(og, wout_ref[...], LAST, preferred_element_type=F32)
    dg = dg.astype(BF16).astype(F32)
    dx_s[rows, :width] = (dg * xh * dsil_s[rows, :width].astype(F32)).astype(BF16)
    dxh = dg * gate
    m1 = jnp.mean(dxh, axis=-1, keepdims=True)
    m2 = jnp.mean(dxh * xh, axis=-1, keepdims=True)
    do_s[rows, :] = (rs * (dxh - m1 - xh * m2)).astype(BF16)


def attend_back(h, qkv_s, kv_t, p_s, d_s, do_s, dsil_s, dx_s, dq_t, blocks, width):
    hc = slice(h * 128, (h + 1) * 128)

    def put(block, part, grad):
        cols = slice(part * width + h * 128, part * width + (h + 1) * 128)
        rows = slice(block * B, (block + 1) * B)
        dx_s[rows, cols] = (
            grad.astype(BF16).astype(F32) * dsil_s[rows, cols].astype(F32)
        ).astype(BF16)

    order = pairs(blocks)
    scale = 0.5 / math.sqrt(128) / MOST
    for k in range(blocks):
        dv = dk = None
        vv = qkv_s[0, k * B : (k + 1) * B, hc]
        for q in range(k, min(k + MOST // B, blocks - 1) + 1):
            i = order.index((q, k))
            do = do_s[q * B : (q + 1) * B, hc]
            dp = lax.dot_general(vv, do, LAST, preferred_element_type=F32).astype(BF16)
            ds = dp * d_s[h, i]
            dv1 = jnp.dot(p_s[h, i], do, preferred_element_type=F32)
            dk1 = jnp.dot(ds, qkv_s[1, q * B : (q + 1) * B, hc], preferred_element_type=F32)
            dv = dv1 if dv is None else dv + dv1
            dk = dk1 if dk is None else dk + dk1
            dq1 = jnp.dot(kv_t[0, hc, k * B : (k + 1) * B], ds, preferred_element_type=F32)
            at = slice(q * B, (q + 1) * B)
            if k == max(0, q - MOST // B):
                dq_t[:, at] = dq1
            else:
                dq_t[:, at] += dq1
        put(k, 1, dv * (1.0 / MOST))
        put(k, 3, dk * scale)
    for q in range(blocks):
        put(q, 2, jnp.transpose(dq_t[:, q * B : (q + 1) * B] * scale))


def event_back(r, dx_s, win_ref, normed_s, rstd_s, og_ref, eg_s):
    rows = rows_at(r)
    g = lax.dot_general(dx_s[rows, :], win_ref[...], LAST, preferred_element_type=F32)
    g = g.astype(BF16).astype(F32)
    xh = normed_s[rows, :].astype(F32)
    m1 = jnp.mean(g, axis=-1, keepdims=True)
    m2 = jnp.mean(g * xh, axis=-1, keepdims=True)
    de = (rstd_s[rows, :] * (g - m1 - xh * m2)).astype(BF16)
    eg_s[rows, :] = (de.astype(F32) + og_ref[rows, :].astype(F32)).astype(BF16)


def row_starts(len_ref, blocks):
    ends, at = [], jnp.int32(0)
    for s in range(len_ref.shape[1]):
        at = at + len_ref[0, s]
        ends.append(at)
    starts = []
    for q in range(blocks):
        place = lax.broadcasted_iota(jnp.int32, (1, B), 1) + q * B
        start = jnp.zeros((1, B), jnp.int32)
        for e in ends:
            start = jnp.where(place >= e, e, start)
        starts.append(start)
    return starts


def compute_scratch(tokens, width, slots):
    n = len(pairs(tokens // B))
    heads = width // 128
    return [
        pltpu.VMEM((tokens, width), BF16),
        pltpu.VMEM((slots, tokens), BF16),
        pltpu.VMEM((tokens, width), BF16),
        pltpu.VMEM((width, tokens), BF16),
        pltpu.VMEM((tokens, 1), F32),
        pltpu.VMEM((tokens, width), F32),
        pltpu.VMEM((tokens, 4 * width), BF16),
        pltpu.VMEM((3, tokens, width), BF16),
        pltpu.VMEM((2, width, tokens), BF16),
        pltpu.VMEM((width, tokens), F32),
        pltpu.VMEM((heads, n, B, B), BF16),
        pltpu.VMEM((heads, n, B, B), BF16),
        pltpu.VMEM((width, tokens), BF16),
        pltpu.VMEM((tokens, 4 * width), BF16),
        pltpu.VMEM((tokens, width), BF16),
        pltpu.VMEM((128, tokens), F32),
        pltpu.VMEM((tokens, width), BF16),
    ]


MESH = pl.DeviceIdType.MESH


def remote(src, dst, send_sem, recv_sem, emb, seq):
    return pltpu.make_async_remote_copy(
        src_ref=src, dst_ref=dst, send_sem=send_sem, recv_sem=recv_sem,
        device_id=(emb, seq), device_id_type=MESH,
    )


def rows_of(at, count):
    return pl.ds(pl.multiple_of(at * count, count), count)


def greet(peers):
    barrier = pltpu.get_barrier_semaphore()
    for emb, seq in peers:
        pl.semaphore_signal(barrier, inc=1, device_id=(emb, seq), device_id_type=MESH)
    pl.semaphore_wait(barrier, len(peers))


class Summed:
    def __init__(self, e, s, base, units, g_s, sum_s, bufs, sems):
        self.e, self.s = e, s
        self.c, self.x, self.z = lax.rem(e, 2), lax.rem(e // 2, 4), e // 8
        self.chip = e // 2
        self.other = e + 1 - 2 * self.c
        self.base, self.half, self.piece = base, units // 2, units // 32
        self.g_s, self.sum_s = g_s, sum_s
        self.half_s, self.pair_s, self.b1, self.b3 = bufs
        (self.many_send, self.many_recv, self.few_send, self.few_recv,
         self.wide_send, self.wide_recv) = sems

    def chips(self, t):
        z = lax.rem(self.z + t, 4)
        return [z * 4 + lax.rem(self.x + u, 4) for u in range(0 if t else 1, 4)]

    def line(self, t):
        return lax.rem(self.z + t, 4) * 4 * self.piece

    def halve(self, t):
        src = self.g_s.at[pl.ds(self.base + (1 - self.c) * self.half + self.line(t), 4 * self.piece)]
        dst = self.pair_s.at[pl.ds(self.line(t), 4 * self.piece)]
        return remote(src, dst, self.few_send.at[0, t], self.few_recv.at[0, t], self.other, self.s)

    def spread(self, to):
        return remote(self.half_s.at[pl.ds(to * self.piece, self.piece)], self.b1.at[self.chip],
                      self.many_send.at[0, to], self.many_recv.at[0, self.chip],
                      to * 2 + self.c, self.s)

    def spread_from(self, frm):
        return remote(self.half_s.at[pl.ds(0, self.piece)], self.b1.at[frm],
                      self.many_send.at[0, frm], self.many_recv.at[0, frm],
                      frm * 2 + self.c, self.s)

    def gather3(self, d):
        ref = self.b3.at[self.s]
        return remote(ref, ref, self.few_send.at[1, d], self.few_recv.at[1, d],
                      self.e, lax.rem(self.s + d, 4))

    def own(self, dz, dx, k):
        chip = lax.rem(self.z + dz, 4) * 4 + lax.rem(self.x + dx, 4)
        size = self.piece // 2
        at = self.base + self.c * self.half + chip * self.piece + k * size
        return self.sum_s.at[pl.ds(at, size)]

    def chip_at(self, dz, dx):
        return (lax.rem(self.z + dz, 4) * 4 + lax.rem(self.x + dx, 4)) * 2 + self.c

    def back1(self, k, d):
        ref = self.own(0, 0, k)
        to = self.chip_at(0, d) if k else self.chip_at(d, 0)
        return remote(ref, ref, self.wide_send.at[k, 4, d], self.wide_recv.at[k, 4, d], to, self.s)

    def back2(self, k, i, d):
        ref = self.own(0, i, k) if k else self.own(i, 0, k)
        to = self.chip_at(d, 0) if k else self.chip_at(0, d)
        return remote(ref, ref, self.wide_send.at[k, i, d], self.wide_recv.at[k, i, d], to, self.s)

    def join(self, t):
        ref = self.sum_s.at[pl.ds(self.base + self.c * self.half + self.line(t), 4 * self.piece)]
        return remote(ref, ref, self.few_send.at[2, t], self.few_recv.at[2, t], self.other, self.s)

    def step0(self):
        for t in (2, 1, 3, 0):
            self.halve(t).start()

    def step1(self):
        for t in (2, 1, 3, 0):
            self.halve(t).wait_recv()
            part = pl.ds(self.line(t), 4 * self.piece)
            mine = self.g_s[pl.ds(self.base + self.c * self.half + self.line(t), 4 * self.piece)]
            self.half_s[part] = (mine.astype(F32) + self.pair_s[part].astype(F32)).astype(BF16)
            for to in self.chips(t):
                self.spread(to).start()

    def step2(self):
        total = self.half_s[pl.ds(self.chip * self.piece, self.piece)].astype(F32)
        for t in range(4):
            for frm in self.chips(t):
                self.spread_from(frm).wait_recv()
        for t in range(4):
            for frm in self.chips(t):
                total = total + self.b1[frm].astype(F32)
        self.b3[self.s] = total.astype(BF16)
        for d in (2, 1, 3):
            self.gather3(d).start()

    def step3(self):
        for d in range(1, 4):
            self.gather3(d).wait_recv()
        total = self.b3[0].astype(F32)
        for j in range(1, 4):
            total = total + self.b3[j].astype(F32)
        at = self.base + self.c * self.half + self.chip * self.piece
        self.sum_s[pl.ds(at, self.piece)] = total.astype(BF16)
        for k in range(2):
            for d in (2, 1, 3):
                self.back1(k, d).start()
        for k in range(2):
            for d in (2, 1, 3):
                self.back2(k, 0, d).start()

    def step3b(self):
        for i in (1, 3, 2):
            for k in range(2):
                self.back1(k, 4 - i).wait_recv()
                for d in (2, 1, 3):
                    self.back2(k, i, d).start()

    def step4(self):
        for t in (0, 1, 3, 2):
            for d in range(1, 4):
                self.back2(0, t, d).wait_recv()
            if t:
                for i in range(4):
                    self.back2(1, i, 4 - t).wait_recv()
            self.join(t).start()

    def step5(self):
        for t in range(4):
            self.join(t).wait_recv()

    def drain(self):
        for t in range(4):
            self.halve(t).wait_send()
            self.join(t).wait_send()
            for to in self.chips(t):
                self.spread(to).wait_send()
        for d in range(1, 4):
            self.gather3(d).wait_send()
            for k in range(2):
                self.back1(k, d).wait_send()
                for i in range(4):
                    self.back2(k, i, d).wait_send()


PARTS = (256, 256, 128)
BLOCKS = ([(0, i) for i in range(4)] + [(1, i) for i in range(4)]
          + [(0, 4 * part + i) for part in (1, 2, 3) for i in (0, 1)]
          + [(0, 4 * part + 2) for part in (1, 2, 3)] + [(0, 4 * part + 3) for part in (1, 2, 3)])


def whole(n_emb, n_seq, len_ref, asked_ref, ev_ref, table_ref, win_ref, wout_ref, og_ref,
          lo_ref, tg_ref, total_ref,
          idx_ref, tgb_s, req_ref, table_v, rows_v, tab_s, win_s, wout_s, og_s, lo_s, g_s, sum_s, sg_s, all_s,
          bufs_e, bufs_m, bufs_l, load, save, i_send, i_recv, j_send, j_recv, r_send, r_recv, g_send, g_recv,
          y_send, y_recv, z_send, z_recv, many_send, many_recv, few_send, few_recv,
          wide_send, wide_recv,
          events_s, pick_s, normed_s, normed_t, rstd_s, gate_s, dsil_s, qkv_s, kv_t,
          att_t, p_s, d_s, gated_t, dx_s, do_s, dq_t, eg_s):
    e, s = lax.axis_index("emb"), lax.axis_index("seq")
    tokens, width = og_s.shape
    blocks, heads = tokens // B, width // 128
    cap = tab_s.shape[0] // n_emb
    per = 128 // cap
    groups = n_emb // per
    mine, inner = e // per, lax.rem(e, per)
    loads = [pltpu.make_async_copy(a, b, load.at[i]) for i, (a, b) in enumerate(
        ((table_ref, table_v), (win_ref, win_s), (og_ref, og_s), (wout_ref, wout_s)))]
    for copy in loads:
        copy.start()
    greet([(lax.rem(e + d, n_emb), s) for d in range(1, n_emb)]
          + [(e, lax.rem(s + d, n_seq)) for d in range(1, n_seq)])

    def members(j):
        g = lax.rem(mine + j, groups)
        first = 1 if j == 0 else 0
        return g, [g * per + lax.rem(inner + t, per) for t in range(first, per)]

    def ask(to):
        return remote(req_ref.at[to], idx_ref.at[s, e], i_send.at[to], i_recv.at[e], to, s)

    def asked(frm):
        return remote(req_ref.at[frm], idx_ref.at[s, frm], i_send.at[frm], i_recv.at[frm], frm, s)

    rows_asked = asked_ref[...]
    first = (((0,), (0,)), ((), ()))
    spot = jnp.where(lax.broadcasted_iota(jnp.int32, (cap, 128), 1)
                     == lax.broadcasted_iota(jnp.int32, (cap, 128), 0) + cap * inner, 1.0, 0.0)
    low = rows_asked & 127
    high = (rows_asked - low).astype(F32)
    spot = spot.astype(BF16)
    spread_out = (lax.dot_general(high.astype(BF16), spot, first, preferred_element_type=F32)
                  + lax.dot_general(low.astype(F32).astype(BF16), spot, first,
                                    preferred_element_type=F32)).astype(jnp.int32)
    for to in range(n_emb):
        req_ref[to] = spread_out[to : to + 1, :]
    for j in (2, 1, 3, 0):
        for to in members(j)[1]:
            ask(to).start()
    idx_ref[s, e] = req_ref[e]
    shard = table_v.shape[0]
    lane = lax.broadcasted_iota(jnp.int32, (128, shard), 1)

    def answer(to, j):
        return remote(rows_v.at[j, rows_of(lax.rem(to, per), cap)], tab_s.at[rows_of(e, cap)],
                      r_send.at[to], r_recv.at[e], to, s)

    def answered(frm, j):
        return remote(rows_v.at[j, rows_of(lax.rem(frm, per), cap)], tab_s.at[rows_of(frm, cap)],
                      r_send.at[frm], r_recv.at[frm], frm, s)

    def tell(d):
        to = lax.rem(s + d, n_seq)
        return remote(idx_ref.at[s], idx_ref.at[s], j_send.at[d], j_recv.at[d], e, to)

    loads[0].wait()
    for j in (0, 1, 3, 2):
        g, them = members(j)
        for frm in them:
            asked(frm).wait_recv()
        if j == 2:
            for d in range(1, n_seq):
                tell(d).start()
        row = idx_ref[s, g * per]
        for i in range(1, per):
            row = row + idx_ref[s, g * per + i]
        col = jnp.transpose(jnp.broadcast_to(row, (8, 128)))[:, 0:1]
        hot = jnp.where(col == lane, 1.0, 0.0).astype(BF16)
        rows_v[j] = jnp.dot(hot, table_v[...], preferred_element_type=F32).astype(BF16)
        for to in them:
            answer(to, j).start()
        if j == 0:
            tab_s[rows_of(e, cap), :] = rows_v[0, rows_of(inner, cap), :]

    part = shard // n_seq
    sub = lax.broadcasted_iota(jnp.int32, (part, 128), 0) + s * part
    for n in range(n_seq):
        if n:
            tell(n).wait_recv()
        frm = lax.rem(s + 2 * n_seq - n, n_seq)
        for g in range(groups):
            row = idx_ref[frm, g * per]
            for i in range(1, per):
                row = row + idx_ref[frm, g * per + i]
            table_v[n * part : (n + 1) * part, g * 128 : (g + 1) * 128] = jnp.where(
                sub == row, 1.0, 0.0).astype(BF16)
    for j in range(groups):
        for frm in members(j)[1]:
            answered(frm, j).wait_recv()
    for copy in loads[1:]:
        copy.wait()

    expand(ev_ref, tab_s, events_s, pick_s)
    pl.loop(0, blocks)(lambda r: project(
        r, events_s, win_s, normed_s, normed_t, rstd_s, gate_s, dsil_s, qkv_s, kv_t))
    starts = row_starts(len_ref, blocks)
    pl.loop(0, heads)(lambda h: attend(h, starts, qkv_s, kv_t, att_t, p_s, d_s, blocks))
    pl.loop(0, blocks)(lambda r: middle(
        r, att_t, gate_s, dsil_s, events_s, wout_s, og_s, lo_s, gated_t, dx_s, do_s))
    saves = [pltpu.make_async_copy(lo_s, lo_ref, save.at[0])]
    saves[0].start()

    def put_grad(c, val):
        g_s[pl.ds(c * 64, 32)] = val[:, :128].astype(BF16).reshape(32, 16, 128)
        g_s[pl.ds(c * 64 + 32, 32)] = val[:, 128:].astype(BF16).reshape(32, 16, 128)

    for c in range(2):
        put_grad(c, jnp.dot(normed_t[...], dx_s[:, c * B : (c + 1) * B],
                            preferred_element_type=F32))
        put_grad(2 + c, jnp.dot(gated_t[...], og_s[:, c * B : (c + 1) * B],
                                preferred_element_type=F32))
    sums, base = [], 0
    for i, (units, bufs) in enumerate(zip(PARTS, (bufs_e, bufs_m, bufs_l))):
        sems = [sem.at[i] for sem in (
            many_send, many_recv, few_send, few_recv, wide_send, wide_recv)]
        sums.append(Summed(e, s, base, units, g_s, sum_s, bufs, sems))
        base += units
    early, mid, late = sums
    early.step0()

    def back(h):
        attend_back(h, qkv_s, kv_t, p_s, d_s, do_s, dsil_s, dx_s, dq_t, blocks, width)

    def grads_of(first, last):
        for b in range(first, last, 2):
            pair = [BLOCKS[i][1] * 128 for i in range(b, min(b + 2, last))]
            cols = jnp.concatenate([dx_s[:, at : at + 128] for at in pair], axis=1)
            val = jnp.dot(normed_t[...], cols, preferred_element_type=F32).astype(BF16)
            for i in range(len(pair)):
                g_s[(b + i) * 32 : (b + i + 1) * 32] = (
                    val[:, i * 128 : (i + 1) * 128].reshape(32, 16, 128))

    back(0)
    early.step1()
    back(1)
    back(2)
    grads_of(8, 16)
    mid.step0()
    back(3)
    early.step2()
    mid.step1()
    pl.loop(0, blocks)(lambda r: event_back(r, dx_s, win_s, normed_s, rstd_s, og_s, eg_s))
    sg_s[...] = jnp.dot(pick_s[...], eg_s[...], preferred_element_type=F32).astype(BF16)

    def give(to):
        return remote(sg_s.at[rows_of(to, cap)], all_s.at[s, rows_of(e, cap)],
                      g_send.at[to], g_recv.at[e], to, s)

    def given(frm):
        return remote(sg_s.at[rows_of(frm, cap)], all_s.at[s, rows_of(frm, cap)],
                      g_send.at[frm], g_recv.at[frm], frm, s)

    for j in (0, 1, 3, 2):
        for to in members(j)[1]:
            give(to).start()
    all_s[s, rows_of(e, cap), :] = sg_s[rows_of(e, cap), :]
    early.step3()
    grads_of(16, 20)
    late.step0()
    chunk = all_s.shape[1] // groups
    up, down = lax.rem(s + 1, n_seq), lax.rem(s + n_seq - 1, n_seq)

    def pass_on(j, way):
        ref = all_s.at[s, rows_of(lax.rem(mine + j, groups), chunk)]
        return remote(ref, ref, y_send.at[way, j], y_recv.at[way, j], e, down if way else up)

    def relay(j):
        frm, to = (down, up) if j % 2 else (up, down)
        ref = all_s.at[frm, rows_of(lax.rem(mine + j, groups), chunk)]
        return remote(ref, ref, z_send.at[j], z_recv.at[j], e, to)

    def arrived(j):
        for frm in members(j)[1]:
            given(frm).wait_recv()
        for way in range(2):
            pass_on(j, way).start()

    def further(j):
        pass_on(j, 0 if j % 2 else 1).wait_recv()
        relay(j).start()

    def add(n):
        frm = lax.rem(s + 2 * n_seq - n, n_seq)

        @pl.loop(0, blocks)
        def _(r):
            at = pl.ds(pl.multiple_of(n * part + r * B, B), B)
            val = jnp.dot(table_v[at, :], all_s[frm], preferred_element_type=F32)
            if n == 0:
                gate_s[rows_at(r), :] = val
            elif n == 2:
                tgb_s[rows_at(r), :] = (gate_s[rows_at(r), :] + val).astype(BF16)
            else:
                gate_s[rows_at(r), :] += val

    def keep(i):
        rows = pl.ds(sums[i].base, PARTS[i])
        saves.append(pltpu.make_async_copy(sum_s.at[rows], total_ref.at[rows], save.at[2 + i]))
        saves[-1].start()

    arrived(0)
    late.step1()
    early.step3b()
    mid.step2()
    arrived(1)
    further(0)
    late.step2()
    arrived(2)
    early.step4()
    mid.step3()
    further(1)
    late.step3()
    arrived(3)
    mid.step3b()
    further(2)
    late.step3b()
    add(0)
    early.step5()
    keep(0)
    further(3)
    mid.step4()
    late.step4()
    for j in range(groups):
        pass_on(j, 1 if j % 2 else 0).wait_recv()
    add(1)
    add(3)
    mid.step5()
    keep(1)
    late.step5()
    keep(2)
    for j in range(groups):
        relay(j).wait_recv()
    add(2)
    saves.append(pltpu.make_async_copy(tgb_s, tg_ref, save.at[1]))
    saves[-1].start()
    for d in range(1, n_seq):
        tell(d).wait_send()
    for j in range(groups):
        for to in members(j)[1]:
            ask(to).wait_send()
            answer(to, j).wait_send()
            give(to).wait_send()
        relay(j).wait_send()
        for way in range(2):
            pass_on(j, way).wait_send()
    for part in sums:
        part.drain()
    for copy in saves:
        copy.wait()


def layer_grads(lengths, asked, ev, table, win, wout, og, n_emb, n_seq, slots):
    vm = pl.BlockSpec(memory_space=pltpu.VMEM)
    hbm = pl.BlockSpec(memory_space=pl.ANY)
    tokens, width = og.shape
    tile = (16, 128)
    units = 5 * width * width // (16 * 128)
    dma = pltpu.SemaphoreType.DMA

    def sums(n):
        shapes = [(n // 2,), (n // 2,), (16, n // 32), (n_seq, n // 32)]
        return tuple(pltpu.VMEM(shape + tile, BF16) for shape in shapes)

    return pl.pallas_call(
        functools.partial(whole, n_emb, n_seq),
        name="layer",
        out_shape=(
            jax.ShapeDtypeStruct((tokens, width), BF16),
            jax.ShapeDtypeStruct((tokens, width), BF16),
            jax.ShapeDtypeStruct((units,) + tile, BF16),
        ),
        in_specs=[pl.BlockSpec(memory_space=pltpu.SMEM), vm, vm] + [hbm] * 4,
        out_specs=(hbm, hbm, hbm),
        scratch_shapes=[
            pltpu.VMEM((n_seq, n_emb, 1, 128), jnp.int32),
            pltpu.VMEM((tokens, width), BF16),
            pltpu.VMEM((n_emb, 1, 128), jnp.int32),
            pltpu.VMEM(table.shape, BF16),
            pltpu.VMEM((4, 128, width), BF16),
            pltpu.VMEM((slots, width), BF16),
            pltpu.VMEM(win.shape, BF16),
            pltpu.VMEM(wout.shape, BF16),
            pltpu.VMEM(og.shape, BF16),
            pltpu.VMEM(og.shape, BF16),
            pltpu.VMEM((units,) + tile, BF16),
            pltpu.VMEM((units,) + tile, BF16),
            pltpu.VMEM((slots, width), BF16),
            pltpu.VMEM((n_seq, slots, width), BF16),
        ] + [sums(n) for n in PARTS] + [
            dma((4,)), dma((5,)),
            dma((n_emb,)), dma((n_emb,)), dma((n_seq,)), dma((n_seq,)),
            dma((n_emb,)), dma((n_emb,)), dma((n_emb,)), dma((n_emb,)),
            dma((2, 4)), dma((2, 4)), dma((4,)), dma((4,)),
            dma((3, 2, 16)), dma((3, 2, 16)), dma((3, 3, 4)), dma((3, 3, 4)),
            dma((3, 2, 5, 4)), dma((3, 2, 5, 4)),
        ] + compute_scratch(tokens, width, slots),
        compiler_params=pltpu.CompilerParams(
            collective_id=0, has_side_effects=True, vmem_limit_bytes=67043328),
    )(lengths, asked, ev, table, win, wout, og)


def finish(rows_ref, sum_ref, out_ref, tg_ref, wi_ref, wo_ref, lo_ref,
           rows_s, sum_s, lo_s, tg_v, wi_v, wo_v, load, sems):
    width = lo_s.shape[1]
    loads = [pltpu.make_async_copy(a, b, load.at[i]) for i, (a, b) in enumerate(
        ((rows_ref, rows_s), (sum_ref, sum_s), (out_ref, lo_s)))]
    for copy in loads:
        copy.start()
    loads[0].wait()
    tg_v[...] = rows_s[...].astype(F32)
    copies = [pltpu.make_async_copy(tg_v, tg_ref, sems.at[6])]
    copies[-1].start()
    loads[1].wait()
    tall = width // 4
    for r in range(4):
        for b in range(20):
            val = sum_s[b * 32 + r * 8 : b * 32 + r * 8 + 8].reshape(tall, 128).astype(F32)
            rows = slice(r * tall, (r + 1) * tall)
            which, at = BLOCKS[b]
            (wo_v if which else wi_v)[rows, at * 128 : (at + 1) * 128] = val
        copies.append(pltpu.make_async_copy(wi_v.at[rows], wi_ref.at[rows], sems.at[r]))
        copies[-1].start()
    copies.append(pltpu.make_async_copy(wo_v, wo_ref, sems.at[4]))
    copies[-1].start()
    loads[2].wait()
    copies.append(pltpu.make_async_copy(lo_s, lo_ref, sems.at[5]))
    copies[-1].start()
    for copy in copies:
        copy.wait()


def finish_grads(rows, total, out):
    hbm = pl.BlockSpec(memory_space=pl.ANY)
    width = out.shape[1]
    shapes = [(rows.shape, F32), ((width, 4 * width), F32), ((width, width), F32)]
    return pl.pallas_call(
        finish,
        name="finish",
        out_shape=tuple(jax.ShapeDtypeStruct(*a) for a in shapes + [(out.shape, BF16)]),
        in_specs=[hbm] * 3,
        out_specs=(hbm,) * 4,
        scratch_shapes=[pltpu.VMEM(a.shape, BF16) for a in (rows, total, out)]
        + [pltpu.VMEM(*a) for a in shapes]
        + [pltpu.SemaphoreType.DMA((3,)), pltpu.SemaphoreType.DMA((7,))],
        compiler_params=pltpu.CompilerParams(vmem_limit_bytes=67043328),
    )(rows, total, out)


def on_device(item_table, fetch_rows, event_slot, lengths, in_weight, out_weight, out_grad):
    n_emb, n_seq = lax.axis_size("emb"), lax.axis_size("seq")
    cap = fetch_rows.shape[-1]
    layer_out, rows_grad, total = layer_grads(
        lengths, jnp.swapaxes(fetch_rows, 2, 3).reshape(cap, n_emb), event_slot.reshape(-1, 128), item_table,
        in_weight, out_weight, out_grad, n_emb, n_seq, n_emb * cap)
    table_grad, in_total, out_total, layer_out = finish_grads(rows_grad, total, layer_out)
    return layer_out, table_grad, in_total, out_total


def solution(mesh):
    both = P(("emb", "seq"))
    rows = P(("emb", "seq"), None)
    return jax.shard_map(
        on_device,
        mesh=mesh,
        in_specs=(P("emb", None), P("emb", "seq", None, None), both, rows, P(), P(), rows),
        out_specs=(rows, rows, P(), P()),
        check_vma=False,
    )
```

```python
import functools, math
import jax, jax.numpy as jnp
from jax import lax
from jax.experimental import pallas as pl
from jax.experimental.pallas import tpu as pltpu
from jax.sharding import PartitionSpec as P

F32, BF16 = jnp.float32, jnp.bfloat16
EPS = 1e-05
MOST = 512
B = 256
LAST = (((1,), (1,)), ((), ()))


def rows_at(i):
    return pl.ds(pl.multiple_of(i * B, B), B)


def expand(ev_ref, tab_ref, events_s, pick_s):
    slots = tab_ref.shape[0]
    ev = ev_ref[...]
    ev_t = jnp.transpose(ev)
    lane = lax.broadcasted_iota(jnp.int32, (128, slots), 1)
    sub = lax.broadcasted_iota(jnp.int32, (slots, 128), 0)
    for a in range(ev.shape[0]):
        hot = jnp.where(ev_t[:, a : a + 1] == lane, 1.0, 0.0).astype(BF16)
        events_s[128 * a : 128 * a + 128, :] = jnp.dot(
            hot, tab_ref[...], preferred_element_type=F32
        ).astype(BF16)
        pick_s[:, 128 * a : 128 * a + 128] = jnp.where(sub == ev[a : a + 1, :], 1.0, 0.0).astype(
            BF16
        )


def project(r, events_s, win_ref, normed_s, normed_t, rstd_s, gate_s, dsil_s, qkv_s, kv_t):
    rows = rows_at(r)
    width = events_s.shape[1]
    e = events_s[rows, :].astype(F32)
    c = e - jnp.mean(e, axis=-1, keepdims=True)
    rs = lax.rsqrt(jnp.mean(c * c, axis=-1, keepdims=True) + EPS)
    n = (c * rs).astype(BF16)
    normed_s[rows, :] = n
    rstd_s[rows, :] = rs
    normed_t[:, rows] = jnp.transpose(n)
    for b in range(4):
        cols = slice(b * width, (b + 1) * width)
        x = jnp.dot(n, win_ref[:, cols], preferred_element_type=F32)
        hx = 0.5 * x
        t = jnp.tanh(hx)
        u = 1.0 + t
        y = hx * u
        dsil_s[rows, cols] = (0.5 * (u + hx * (1.0 - t * t))).astype(BF16)
        if b == 0:
            gate_s[rows, :] = y
        else:
            yb = y.astype(BF16)
            qkv_s[b - 1, rows, :] = yb
            if b == 1:
                kv_t[1, :, rows] = jnp.transpose(yb)
            elif b == 3:
                kv_t[0, :, rows] = jnp.transpose(yb)


def pairs(blocks):
    back = MOST // B
    return [(q, k) for q in range(blocks) for k in range(max(0, q - back), q + 1)]


def attend(h, starts, qkv_s, kv_t, att_t, p_s, d_s, blocks):
    hc = pl.ds(pl.multiple_of(h * 128, 128), 128)
    lane = lax.broadcasted_iota(jnp.int32, (B, B), 1)
    sub = lax.broadcasted_iota(jnp.int32, (B, B), 0)
    head = 128
    c1 = 0.5 / math.sqrt(head)
    total = None
    for i, (q, k) in enumerate(pairs(blocks)):
        kk = qkv_s[2, k * B : (k + 1) * B, hc]
        qq = qkv_s[1, q * B : (q + 1) * B, hc]
        x = lax.dot_general(kk, qq, LAST, preferred_element_type=F32)
        hh = x * c1
        t = jnp.tanh(hh)
        u = 1.0 + t
        mask = (sub + k * B) >= starts[q]
        if q == k:
            mask = mask & (sub <= lane)
        w = jnp.where(mask, hh * u, 0.0).astype(BF16)
        d = jnp.where(mask, u + hh * (1.0 - t * t), 0.0).astype(BF16)
        p_s[h, i] = w
        d_s[h, i] = d
        o = jnp.dot(kv_t[1, hc, k * B : (k + 1) * B], w, preferred_element_type=F32)
        total = o if k == max(0, q - MOST // B) else total + o
        if q == k:
            att_t[hc, q * B : (q + 1) * B] = total * (1.0 / MOST)


def middle(r, att_t, gate_s, dsil_s, events_s, wout_ref, og_ref, lo_ref, gated_t, dx_s, do_s):
    rows = rows_at(r)
    width = events_s.shape[1]
    a = jnp.transpose(att_t[:, rows])
    c = a - jnp.mean(a, axis=-1, keepdims=True)
    rs = lax.rsqrt(jnp.mean(c * c, axis=-1, keepdims=True) + EPS)
    xh = c * rs
    gate = gate_s[rows, :]
    gated = (xh * gate).astype(BF16)
    out = jnp.dot(gated, wout_ref[...], preferred_element_type=F32)
    lo_ref[rows, :] = (out + events_s[rows, :].astype(F32)).astype(BF16)
    gated_t[:, rows] = jnp.transpose(gated)
    og = og_ref[rows, :]
    dg = lax.dot_general(og, wout_ref[...], LAST, preferred_element_type=F32)
    dg = dg.astype(BF16).astype(F32)
    dx_s[rows, :width] = (dg * xh * dsil_s[rows, :width].astype(F32)).astype(BF16)
    dxh = dg * gate
    m1 = jnp.mean(dxh, axis=-1, keepdims=True)
    m2 = jnp.mean(dxh * xh, axis=-1, keepdims=True)
    do_s[rows, :] = (rs * (dxh - m1 - xh * m2)).astype(BF16)


def attend_back(h, qkv_s, kv_t, p_s, d_s, do_s, dsil_s, dx_s, dq_t, blocks, width):
    hc = slice(h * 128, (h + 1) * 128)

    def put(block, part, grad):
        cols = slice(part * width + h * 128, part * width + (h + 1) * 128)
        rows = slice(block * B, (block + 1) * B)
        dx_s[rows, cols] = (
            grad.astype(BF16).astype(F32) * dsil_s[rows, cols].astype(F32)
        ).astype(BF16)

    order = pairs(blocks)
    scale = 0.5 / math.sqrt(128) / MOST
    for k in range(blocks):
        dv = dk = None
        vv = qkv_s[0, k * B : (k + 1) * B, hc]
        for q in range(k, min(k + MOST // B, blocks - 1) + 1):
            i = order.index((q, k))
            do = do_s[q * B : (q + 1) * B, hc]
            dp = lax.dot_general(vv, do, LAST, preferred_element_type=F32).astype(BF16)
            ds = dp * d_s[h, i]
            dv1 = jnp.dot(p_s[h, i], do, preferred_element_type=F32)
            dk1 = jnp.dot(ds, qkv_s[1, q * B : (q + 1) * B, hc], preferred_element_type=F32)
            dv = dv1 if dv is None else dv + dv1
            dk = dk1 if dk is None else dk + dk1
            dq1 = jnp.dot(kv_t[0, hc, k * B : (k + 1) * B], ds, preferred_element_type=F32)
            at = slice(q * B, (q + 1) * B)
            if k == max(0, q - MOST // B):
                dq_t[:, at] = dq1
            else:
                dq_t[:, at] += dq1
        put(k, 1, dv * (1.0 / MOST))
        put(k, 3, dk * scale)
    for q in range(blocks):
        put(q, 2, jnp.transpose(dq_t[:, q * B : (q + 1) * B] * scale))


def event_back(r, dx_s, win_ref, normed_s, rstd_s, og_ref, eg_s):
    rows = rows_at(r)
    g = lax.dot_general(dx_s[rows, :], win_ref[...], LAST, preferred_element_type=F32)
    g = g.astype(BF16).astype(F32)
    xh = normed_s[rows, :].astype(F32)
    m1 = jnp.mean(g, axis=-1, keepdims=True)
    m2 = jnp.mean(g * xh, axis=-1, keepdims=True)
    de = (rstd_s[rows, :] * (g - m1 - xh * m2)).astype(BF16)
    eg_s[rows, :] = (de.astype(F32) + og_ref[rows, :].astype(F32)).astype(BF16)


def row_starts(len_ref, blocks):
    ends, at = [], jnp.int32(0)
    for s in range(len_ref.shape[1]):
        at = at + len_ref[0, s]
        ends.append(at)
    starts = []
    for q in range(blocks):
        place = lax.broadcasted_iota(jnp.int32, (1, B), 1) + q * B
        start = jnp.zeros((1, B), jnp.int32)
        for e in ends:
            start = jnp.where(place >= e, e, start)
        starts.append(start)
    return starts


def compute_scratch(tokens, width, slots):
    n = len(pairs(tokens // B))
    heads = width // 128
    return [
        pltpu.VMEM((tokens, width), BF16),
        pltpu.VMEM((slots, tokens), BF16),
        pltpu.VMEM((tokens, width), BF16),
        pltpu.VMEM((width, tokens), BF16),
        pltpu.VMEM((tokens, 1), F32),
        pltpu.VMEM((tokens, width), F32),
        pltpu.VMEM((tokens, 4 * width), BF16),
        pltpu.VMEM((3, tokens, width), BF16),
        pltpu.VMEM((2, width, tokens), BF16),
        pltpu.VMEM((width, tokens), F32),
        pltpu.VMEM((heads, n, B, B), BF16),
        pltpu.VMEM((heads, n, B, B), BF16),
        pltpu.VMEM((width, tokens), BF16),
        pltpu.VMEM((tokens, 4 * width), BF16),
        pltpu.VMEM((tokens, width), BF16),
        pltpu.VMEM((128, tokens), F32),
        pltpu.VMEM((tokens, width), BF16),
    ]


MESH = pl.DeviceIdType.MESH


def remote(src, dst, send_sem, recv_sem, emb, seq):
    return pltpu.make_async_remote_copy(
        src_ref=src, dst_ref=dst, send_sem=send_sem, recv_sem=recv_sem,
        device_id=(emb, seq), device_id_type=MESH,
    )


def rows_of(at, count):
    return pl.ds(pl.multiple_of(at * count, count), count)


def greet(peers):
    barrier = pltpu.get_barrier_semaphore()
    for emb, seq in peers:
        pl.semaphore_signal(barrier, inc=1, device_id=(emb, seq), device_id_type=MESH)
    pl.semaphore_wait(barrier, len(peers))


class Summed:
    def __init__(self, e, s, base, units, g_s, sum_s, bufs, sems):
        self.e, self.s = e, s
        self.c, self.x, self.z = lax.rem(e, 2), lax.rem(e // 2, 4), e // 8
        self.chip = e // 2
        self.other = e + 1 - 2 * self.c
        self.base, self.half, self.piece = base, units // 2, units // 32
        self.g_s, self.sum_s = g_s, sum_s
        self.half_s, self.pair_s, self.b1, self.b3 = bufs
        (self.many_send, self.many_recv, self.few_send, self.few_recv,
         self.wide_send, self.wide_recv) = sems

    def chips(self, t):
        z = lax.rem(self.z + t, 4)
        return [z * 4 + lax.rem(self.x + u, 4) for u in range(0 if t else 1, 4)]

    def line(self, t):
        return lax.rem(self.z + t, 4) * 4 * self.piece

    def halve(self, t):
        src = self.g_s.at[pl.ds(self.base + (1 - self.c) * self.half + self.line(t), 4 * self.piece)]
        dst = self.pair_s.at[pl.ds(self.line(t), 4 * self.piece)]
        return remote(src, dst, self.few_send.at[0, t], self.few_recv.at[0, t], self.other, self.s)

    def spread(self, to):
        return remote(self.half_s.at[pl.ds(to * self.piece, self.piece)], self.b1.at[self.chip],
                      self.many_send.at[0, to], self.many_recv.at[0, self.chip],
                      to * 2 + self.c, self.s)

    def spread_from(self, frm):
        return remote(self.half_s.at[pl.ds(0, self.piece)], self.b1.at[frm],
                      self.many_send.at[0, frm], self.many_recv.at[0, frm],
                      frm * 2 + self.c, self.s)

    def gather3(self, d):
        ref = self.b3.at[self.s]
        return remote(ref, ref, self.few_send.at[1, d], self.few_recv.at[1, d],
                      self.e, lax.rem(self.s + d, 4))

    def own(self, dz, dx, k):
        chip = lax.rem(self.z + dz, 4) * 4 + lax.rem(self.x + dx, 4)
        size = self.piece // 2
        at = self.base + self.c * self.half + chip * self.piece + k * size
        return self.sum_s.at[pl.ds(at, size)]

    def chip_at(self, dz, dx):
        return (lax.rem(self.z + dz, 4) * 4 + lax.rem(self.x + dx, 4)) * 2 + self.c

    def back1(self, k, d):
        ref = self.own(0, 0, k)
        to = self.chip_at(0, d) if k else self.chip_at(d, 0)
        return remote(ref, ref, self.wide_send.at[k, 4, d], self.wide_recv.at[k, 4, d], to, self.s)

    def back2(self, k, i, d):
        ref = self.own(0, i, k) if k else self.own(i, 0, k)
        to = self.chip_at(d, 0) if k else self.chip_at(0, d)
        return remote(ref, ref, self.wide_send.at[k, i, d], self.wide_recv.at[k, i, d], to, self.s)

    def join(self, t):
        ref = self.sum_s.at[pl.ds(self.base + self.c * self.half + self.line(t), 4 * self.piece)]
        return remote(ref, ref, self.few_send.at[2, t], self.few_recv.at[2, t], self.other, self.s)

    def step0(self):
        for t in (2, 1, 3, 0):
            self.halve(t).start()

    def step1(self):
        for t in (2, 1, 3, 0):
            self.halve(t).wait_recv()
            part = pl.ds(self.line(t), 4 * self.piece)
            mine = self.g_s[pl.ds(self.base + self.c * self.half + self.line(t), 4 * self.piece)]
            self.half_s[part] = (mine.astype(F32) + self.pair_s[part].astype(F32)).astype(BF16)
            for to in self.chips(t):
                self.spread(to).start()

    def step2(self):
        total = self.half_s[pl.ds(self.chip * self.piece, self.piece)].astype(F32)
        for t in range(4):
            for frm in self.chips(t):
                self.spread_from(frm).wait_recv()
        for t in range(4):
            for frm in self.chips(t):
                total = total + self.b1[frm].astype(F32)
        self.b3[self.s] = total.astype(BF16)
        for d in (2, 1, 3):
            self.gather3(d).start()

    def step3(self):
        for d in range(1, 4):
            self.gather3(d).wait_recv()
        total = self.b3[0].astype(F32)
        for j in range(1, 4):
            total = total + self.b3[j].astype(F32)
        at = self.base + self.c * self.half + self.chip * self.piece
        self.sum_s[pl.ds(at, self.piece)] = total.astype(BF16)
        for k in range(2):
            for d in (2, 1, 3):
                self.back1(k, d).start()
        for k in range(2):
            for d in (2, 1, 3):
                self.back2(k, 0, d).start()

    def step3b(self):
        for i in (1, 3, 2):
            for k in range(2):
                self.back1(k, 4 - i).wait_recv()
                for d in (2, 1, 3):
                    self.back2(k, i, d).start()

    def step4(self):
        for t in (0, 1, 3, 2):
            for d in range(1, 4):
                self.back2(0, t, d).wait_recv()
            if t:
                for i in range(4):
                    self.back2(1, i, 4 - t).wait_recv()
            self.join(t).start()

    def step5(self):
        for t in range(4):
            self.join(t).wait_recv()

    def drain(self):
        for t in range(4):
            self.halve(t).wait_send()
            self.join(t).wait_send()
            for to in self.chips(t):
                self.spread(to).wait_send()
        for d in range(1, 4):
            self.gather3(d).wait_send()
            for k in range(2):
                self.back1(k, d).wait_send()
                for i in range(4):
                    self.back2(k, i, d).wait_send()


PARTS = (256, 256, 128)
BLOCKS = ([(0, i) for i in range(4)] + [(1, i) for i in range(4)]
          + [(0, 4 * part + i) for part in (1, 2, 3) for i in (0, 1)]
          + [(0, 4 * part + 2) for part in (1, 2, 3)] + [(0, 4 * part + 3) for part in (1, 2, 3)])


def whole(n_emb, n_seq, len_ref, asked_ref, ev_ref, table_ref, win_ref, wout_ref, og_ref,
          lo_ref, tg_ref, total_ref,
          idx_ref, tgb_s, req_ref, table_v, rows_v, tab_s, win_s, wout_s, og_s, lo_s, g_s, sum_s, sg_s, all_s,
          bufs_e, bufs_m, bufs_l, load, save, i_send, i_recv, j_send, j_recv, r_send, r_recv, g_send, g_recv,
          y_send, y_recv, z_send, z_recv, many_send, many_recv, few_send, few_recv,
          wide_send, wide_recv,
          events_s, pick_s, normed_s, normed_t, rstd_s, gate_s, dsil_s, qkv_s, kv_t,
          att_t, p_s, d_s, gated_t, dx_s, do_s, dq_t, eg_s):
    e, s = lax.axis_index("emb"), lax.axis_index("seq")
    tokens, width = og_s.shape
    blocks, heads = tokens // B, width // 128
    cap = tab_s.shape[0] // n_emb
    per = 128 // cap
    groups = n_emb // per
    mine, inner = e // per, lax.rem(e, per)
    loads = [pltpu.make_async_copy(a, b, load.at[i]) for i, (a, b) in enumerate(
        ((table_ref, table_v), (win_ref, win_s), (og_ref, og_s), (wout_ref, wout_s)))]
    for copy in loads:
        copy.start()
    greet([(lax.rem(e + d, n_emb), s) for d in range(1, n_emb)]
          + [(e, lax.rem(s + d, n_seq)) for d in range(1, n_seq)])

    def members(j):
        g = lax.rem(mine + j, groups)
        first = 1 if j == 0 else 0
        return g, [g * per + lax.rem(inner + t, per) for t in range(first, per)]

    def ask(to):
        return remote(req_ref.at[to], idx_ref.at[s, e], i_send.at[to], i_recv.at[e], to, s)

    def asked(frm):
        return remote(req_ref.at[frm], idx_ref.at[s, frm], i_send.at[frm], i_recv.at[frm], frm, s)

    rows_asked = asked_ref[...]
    first = (((0,), (0,)), ((), ()))
    spot = jnp.where(lax.broadcasted_iota(jnp.int32, (cap, 128), 1)
                     == lax.broadcasted_iota(jnp.int32, (cap, 128), 0) + cap * inner, 1.0, 0.0)
    low = rows_asked & 127
    high = (rows_asked - low).astype(F32)
    spot = spot.astype(BF16)
    spread_out = (lax.dot_general(high.astype(BF16), spot, first, preferred_element_type=F32)
                  + lax.dot_general(low.astype(F32).astype(BF16), spot, first,
                                    preferred_element_type=F32)).astype(jnp.int32)
    for to in range(n_emb):
        req_ref[to] = spread_out[to : to + 1, :]
    for j in (2, 1, 3, 0):
        for to in members(j)[1]:
            ask(to).start()
    idx_ref[s, e] = req_ref[e]
    shard = table_v.shape[0]
    lane = lax.broadcasted_iota(jnp.int32, (128, shard), 1)

    def answer(to, j):
        return remote(rows_v.at[j, rows_of(lax.rem(to, per), cap)], tab_s.at[rows_of(e, cap)],
                      r_send.at[to], r_recv.at[e], to, s)

    def answered(frm, j):
        return remote(rows_v.at[j, rows_of(lax.rem(frm, per), cap)], tab_s.at[rows_of(frm, cap)],
                      r_send.at[frm], r_recv.at[frm], frm, s)

    def tell(d):
        to = lax.rem(s + d, n_seq)
        return remote(idx_ref.at[s], idx_ref.at[s], j_send.at[d], j_recv.at[d], e, to)

    loads[0].wait()
    for j in (0, 1, 3, 2):
        g, them = members(j)
        for frm in them:
            asked(frm).wait_recv()
        if j == 2:
            for d in range(1, n_seq):
                tell(d).start()
        row = idx_ref[s, g * per]
        for i in range(1, per):
            row = row + idx_ref[s, g * per + i]
        col = jnp.transpose(jnp.broadcast_to(row, (8, 128)))[:, 0:1]
        hot = jnp.where(col == lane, 1.0, 0.0).astype(BF16)
        rows_v[j] = jnp.dot(hot, table_v[...], preferred_element_type=F32).astype(BF16)
        for to in them:
            answer(to, j).start()
        if j == 0:
            tab_s[rows_of(e, cap), :] = rows_v[0, rows_of(inner, cap), :]

    part = shard // n_seq
    sub = lax.broadcasted_iota(jnp.int32, (part, 128), 0) + s * part
    for n in range(n_seq):
        if n:
            tell(n).wait_recv()
        frm = lax.rem(s + 2 * n_seq - n, n_seq)
        for g in range(groups):
            row = idx_ref[frm, g * per]
            for i in range(1, per):
                row = row + idx_ref[frm, g * per + i]
            table_v[n * part : (n + 1) * part, g * 128 : (g + 1) * 128] = jnp.where(
                sub == row, 1.0, 0.0).astype(BF16)
    for j in range(groups):
        for frm in members(j)[1]:
            answered(frm, j).wait_recv()
    for copy in loads[1:]:
        copy.wait()

    expand(ev_ref, tab_s, events_s, pick_s)
    pl.loop(0, blocks)(lambda r: project(
        r, events_s, win_s, normed_s, normed_t, rstd_s, gate_s, dsil_s, qkv_s, kv_t))
    starts = row_starts(len_ref, blocks)
    pl.loop(0, heads)(lambda h: attend(h, starts, qkv_s, kv_t, att_t, p_s, d_s, blocks))
    pl.loop(0, blocks)(lambda r: middle(
        r, att_t, gate_s, dsil_s, events_s, wout_s, og_s, lo_s, gated_t, dx_s, do_s))
    saves = [pltpu.make_async_copy(lo_s, lo_ref, save.at[0])]
    saves[0].start()

    def put_grad(c, val):
        g_s[pl.ds(c * 64, 32)] = val[:, :128].astype(BF16).reshape(32, 16, 128)
        g_s[pl.ds(c * 64 + 32, 32)] = val[:, 128:].astype(BF16).reshape(32, 16, 128)

    for c in range(2):
        put_grad(c, jnp.dot(normed_t[...], dx_s[:, c * B : (c + 1) * B],
                            preferred_element_type=F32))
        put_grad(2 + c, jnp.dot(gated_t[...], og_s[:, c * B : (c + 1) * B],
                                preferred_element_type=F32))
    sums, base = [], 0
    for i, (units, bufs) in enumerate(zip(PARTS, (bufs_e, bufs_m, bufs_l))):
        sems = [sem.at[i] for sem in (
            many_send, many_recv, few_send, few_recv, wide_send, wide_recv)]
        sums.append(Summed(e, s, base, units, g_s, sum_s, bufs, sems))
        base += units
    early, mid, late = sums
    early.step0()

    def back(h):
        attend_back(h, qkv_s, kv_t, p_s, d_s, do_s, dsil_s, dx_s, dq_t, blocks, width)

    def grads_of(first, last):
        for b in range(first, last, 2):
            pair = [BLOCKS[i][1] * 128 for i in range(b, min(b + 2, last))]
            cols = jnp.concatenate([dx_s[:, at : at + 128] for at in pair], axis=1)
            val = jnp.dot(normed_t[...], cols, preferred_element_type=F32).astype(BF16)
            for i in range(len(pair)):
                g_s[(b + i) * 32 : (b + i + 1) * 32] = (
                    val[:, i * 128 : (i + 1) * 128].reshape(32, 16, 128))

    back(0)
    early.step1()
    back(1)
    back(2)
    grads_of(8, 16)
    mid.step0()
    back(3)
    grads_of(16, 20)
    late.step0()
    early.step2()
    mid.step1()
    pl.loop(0, blocks)(lambda r: event_back(r, dx_s, win_s, normed_s, rstd_s, og_s, eg_s))
    early.step3()
    late.step1()
    sg_s[...] = jnp.dot(pick_s[...], eg_s[...], preferred_element_type=F32).astype(BF16)

    def give(to):
        return remote(sg_s.at[rows_of(to, cap)], all_s.at[s, rows_of(e, cap)],
                      g_send.at[to], g_recv.at[e], to, s)

    def given(frm):
        return remote(sg_s.at[rows_of(frm, cap)], all_s.at[s, rows_of(frm, cap)],
                      g_send.at[frm], g_recv.at[frm], frm, s)

    for j in (0, 1, 3, 2):
        for to in members(j)[1]:
            give(to).start()
    all_s[s, rows_of(e, cap), :] = sg_s[rows_of(e, cap), :]
    chunk = all_s.shape[1] // groups
    up, down = lax.rem(s + 1, n_seq), lax.rem(s + n_seq - 1, n_seq)

    def pass_on(j, way):
        ref = all_s.at[s, rows_of(lax.rem(mine + j, groups), chunk)]
        return remote(ref, ref, y_send.at[way, j], y_recv.at[way, j], e, down if way else up)

    def relay(j):
        frm, to = (down, up) if j % 2 else (up, down)
        ref = all_s.at[frm, rows_of(lax.rem(mine + j, groups), chunk)]
        return remote(ref, ref, z_send.at[j], z_recv.at[j], e, to)

    def arrived(j):
        for frm in members(j)[1]:
            given(frm).wait_recv()
        for way in range(2):
            pass_on(j, way).start()

    def further(j):
        pass_on(j, 0 if j % 2 else 1).wait_recv()
        relay(j).start()

    def add(n):
        frm = lax.rem(s + 2 * n_seq - n, n_seq)

        @pl.loop(0, blocks)
        def _(r):
            at = pl.ds(pl.multiple_of(n * part + r * B, B), B)
            val = jnp.dot(table_v[at, :], all_s[frm], preferred_element_type=F32)
            if n == 0:
                gate_s[rows_at(r), :] = val
            elif n == 2:
                tgb_s[rows_at(r), :] = (gate_s[rows_at(r), :] + val).astype(BF16)
            else:
                gate_s[rows_at(r), :] += val

    def keep(i):
        rows = pl.ds(sums[i].base, PARTS[i])
        saves.append(pltpu.make_async_copy(sum_s.at[rows], total_ref.at[rows], save.at[2 + i]))
        saves[-1].start()

    mid.step2()
    early.step3b()
    arrived(0)
    late.step2()
    arrived(1)
    mid.step3()
    further(0)
    early.step4()
    arrived(2)
    late.step3()
    mid.step3b()
    further(1)
    arrived(3)
    early.step5()
    keep(0)
    late.step3b()
    mid.step4()
    further(2)
    add(0)
    late.step4()
    further(3)
    for j in range(groups):
        pass_on(j, 1 if j % 2 else 0).wait_recv()
    add(1)
    add(3)
    mid.step5()
    keep(1)
    late.step5()
    keep(2)
    for j in range(groups):
        relay(j).wait_recv()
    add(2)
    saves.append(pltpu.make_async_copy(tgb_s, tg_ref, save.at[1]))
    saves[-1].start()
    for d in range(1, n_seq):
        tell(d).wait_send()
    for j in range(groups):
        for to in members(j)[1]:
            ask(to).wait_send()
            answer(to, j).wait_send()
            give(to).wait_send()
        relay(j).wait_send()
        for way in range(2):
            pass_on(j, way).wait_send()
    for part in sums:
        part.drain()
    for copy in saves:
        copy.wait()


def layer_grads(lengths, asked, ev, table, win, wout, og, n_emb, n_seq, slots):
    vm = pl.BlockSpec(memory_space=pltpu.VMEM)
    hbm = pl.BlockSpec(memory_space=pl.ANY)
    tokens, width = og.shape
    tile = (16, 128)
    units = 5 * width * width // (16 * 128)
    dma = pltpu.SemaphoreType.DMA

    def sums(n):
        shapes = [(n // 2,), (n // 2,), (16, n // 32), (n_seq, n // 32)]
        return tuple(pltpu.VMEM(shape + tile, BF16) for shape in shapes)

    return pl.pallas_call(
        functools.partial(whole, n_emb, n_seq),
        name="layer",
        out_shape=(
            jax.ShapeDtypeStruct((tokens, width), BF16),
            jax.ShapeDtypeStruct((tokens, width), BF16),
            jax.ShapeDtypeStruct((units,) + tile, BF16),
        ),
        in_specs=[pl.BlockSpec(memory_space=pltpu.SMEM), vm, vm] + [hbm] * 4,
        out_specs=(hbm, hbm, hbm),
        scratch_shapes=[
            pltpu.VMEM((n_seq, n_emb, 1, 128), jnp.int32),
            pltpu.VMEM((tokens, width), BF16),
            pltpu.VMEM((n_emb, 1, 128), jnp.int32),
            pltpu.VMEM(table.shape, BF16),
            pltpu.VMEM((4, 128, width), BF16),
            pltpu.VMEM((slots, width), BF16),
            pltpu.VMEM(win.shape, BF16),
            pltpu.VMEM(wout.shape, BF16),
            pltpu.VMEM(og.shape, BF16),
            pltpu.VMEM(og.shape, BF16),
            pltpu.VMEM((units,) + tile, BF16),
            pltpu.VMEM((units,) + tile, BF16),
            pltpu.VMEM((slots, width), BF16),
            pltpu.VMEM((n_seq, slots, width), BF16),
        ] + [sums(n) for n in PARTS] + [
            dma((4,)), dma((5,)),
            dma((n_emb,)), dma((n_emb,)), dma((n_seq,)), dma((n_seq,)),
            dma((n_emb,)), dma((n_emb,)), dma((n_emb,)), dma((n_emb,)),
            dma((2, 4)), dma((2, 4)), dma((4,)), dma((4,)),
            dma((3, 2, 16)), dma((3, 2, 16)), dma((3, 3, 4)), dma((3, 3, 4)),
            dma((3, 2, 5, 4)), dma((3, 2, 5, 4)),
        ] + compute_scratch(tokens, width, slots),
        compiler_params=pltpu.CompilerParams(
            collective_id=0, has_side_effects=True, vmem_limit_bytes=67043328),
    )(lengths, asked, ev, table, win, wout, og)


def finish(rows_ref, sum_ref, out_ref, tg_ref, wi_ref, wo_ref, lo_ref,
           rows_s, sum_s, lo_s, tg_v, wi_v, wo_v, load, sems):
    width = lo_s.shape[1]
    loads = [pltpu.make_async_copy(a, b, load.at[i]) for i, (a, b) in enumerate(
        ((rows_ref, rows_s), (sum_ref, sum_s), (out_ref, lo_s)))]
    for copy in loads:
        copy.start()
    loads[0].wait()
    tg_v[...] = rows_s[...].astype(F32)
    copies = [pltpu.make_async_copy(tg_v, tg_ref, sems.at[6])]
    copies[-1].start()
    loads[1].wait()
    tall = width // 4
    for r in range(4):
        for b in range(20):
            val = sum_s[b * 32 + r * 8 : b * 32 + r * 8 + 8].reshape(tall, 128).astype(F32)
            rows = slice(r * tall, (r + 1) * tall)
            which, at = BLOCKS[b]
            (wo_v if which else wi_v)[rows, at * 128 : (at + 1) * 128] = val
        copies.append(pltpu.make_async_copy(wi_v.at[rows], wi_ref.at[rows], sems.at[r]))
        copies[-1].start()
    copies.append(pltpu.make_async_copy(wo_v, wo_ref, sems.at[4]))
    copies[-1].start()
    loads[2].wait()
    copies.append(pltpu.make_async_copy(lo_s, lo_ref, sems.at[5]))
    copies[-1].start()
    for copy in copies:
        copy.wait()


def finish_grads(rows, total, out):
    hbm = pl.BlockSpec(memory_space=pl.ANY)
    width = out.shape[1]
    shapes = [(rows.shape, F32), ((width, 4 * width), F32), ((width, width), F32)]
    return pl.pallas_call(
        finish,
        name="finish",
        out_shape=tuple(jax.ShapeDtypeStruct(*a) for a in shapes + [(out.shape, BF16)]),
        in_specs=[hbm] * 3,
        out_specs=(hbm,) * 4,
        scratch_shapes=[pltpu.VMEM(a.shape, BF16) for a in (rows, total, out)]
        + [pltpu.VMEM(*a) for a in shapes]
        + [pltpu.SemaphoreType.DMA((3,)), pltpu.SemaphoreType.DMA((7,))],
        compiler_params=pltpu.CompilerParams(vmem_limit_bytes=67043328),
    )(rows, total, out)


def on_device(item_table, fetch_rows, event_slot, lengths, in_weight, out_weight, out_grad):
    n_emb, n_seq = lax.axis_size("emb"), lax.axis_size("seq")
    cap = fetch_rows.shape[-1]
    layer_out, rows_grad, total = layer_grads(
        lengths, jnp.swapaxes(fetch_rows, 2, 3).reshape(cap, n_emb), event_slot.reshape(-1, 128), item_table,
        in_weight, out_weight, out_grad, n_emb, n_seq, n_emb * cap)
    table_grad, in_total, out_total, layer_out = finish_grads(rows_grad, total, layer_out)
    return layer_out, table_grad, in_total, out_total


def solution(mesh):
    both = P(("emb", "seq"))
    rows = P(("emb", "seq"), None)
    return jax.shard_map(
        on_device,
        mesh=mesh,
        in_specs=(P("emb", None), P("emb", "seq", None, None), both, rows, P(), P(), rows),
        out_specs=(rows, rows, P(), P()),
        check_vma=False,
    )
```
